32 devices in a mesh: rows: 8 (over y, x, core), cols: 4 (over z).
Axes of the slice: x: 2, y: 2, z: 4, core: 2. Of those that a mesh axis runs over, the one named last changes fastest.
Arguments:
- token_ids: int32 [16, 2048], P('rows', 'cols'), may hold values from 0 to 131071, as said below
- lengths: int32 [16], P('rows'), may hold values from 1 to 2048
- table: bfloat16 [131072, 512], P('rows', 'cols'), may hold values from -6 to 6
- attn_gain: float32 [512], replicated, may hold values from 0.1 to 1.9
- w_qkv: bfloat16 [512, 1536], replicated, may hold values from -2 to 2
- w_out: bfloat16 [512, 512], replicated, may hold values from -0.25 to 0.25
- mlp_gain: float32 [512], replicated, may hold values from 0.1 to 1.9
- w_in: bfloat16 [512, 4096], replicated, may hold values from -0.25 to 0.25
- w_down: bfloat16 [2048, 512], replicated, may hold values from -0.125 to 0.125
Outputs:
- layer_out: bfloat16 [16, 2048, 512], P('rows', 'cols')
The draws below stay inside these ranges and needn't reach their ends.
Inputs may be any that keep to these rules, and one draw needn't show every extreme that they name: `token_ids`: ids lie in 0 to 131071. In each aligned block of 2 histories (4096 positions) at most 1365 ids fall in any one block of 16384 consecutive table rows, and in every such block of histories some block of table rows receives exactly 1365.
All inputs are finite; a program needn't handle non-finite values.
Results may differ from the reference program's by a relative error of at most 0.012.
Values may be sent and summed in bfloat16 or wider, within the bound.
A program may use at most 192 MiB of HBM per device.

```python
import jax
import jax.numpy as jnp
from jax import lax

D = 512
HEADS = 8
FF = 2048
VOC_DEV = 16384
BD = 2
L = 2048
B = 16
VOCAB = 131072
CAP = 1365


def one_block(key):
    key_hot, key_order, key_shuffle, key_offset = jax.random.split(key, 4)
    block_count = B // BD
    token_count = BD * L
    hot_block = jax.random.randint(key_hot, (), 0, block_count)
    slot_ids = jnp.arange(block_count * CAP, dtype=jnp.int32)
    slot_block = slot_ids // CAP
    order_rank = jax.random.permutation(key_order, block_count * CAP).astype(jnp.int32)
    priority = jnp.where(slot_block == hot_block, 0, 1) * (block_count * CAP) + order_rank
    chosen_order = jnp.argsort(priority)
    chosen_block = slot_block[chosen_order[:token_count]]
    chosen_block = jax.random.permutation(key_shuffle, chosen_block)
    offsets = jax.random.randint(key_offset, (token_count,), 0, VOC_DEV)
    return (chosen_block * VOC_DEV + offsets).astype(jnp.int32).reshape(BD, L)


def draw_token_ids(key, part):
    keys = jax.random.split(jax.random.fold_in(key, 11), B // BD)
    return jax.vmap(one_block)(keys).reshape(B, L)


def draw_w_qkv(key, part):
    key_base = jax.random.fold_in(jax.random.fold_in(key, 23), 0)
    base = jnp.clip(jax.random.normal(key_base, (D, 3 * D), jnp.float32), -5.0, 5.0) / jnp.sqrt(1.0 * D)
    return jnp.clip(base, -2.0, 2.0).astype(jnp.bfloat16)


def touch_ends(drawn, stream_key, low, top_value):
    longest = drawn.shape.index(max(drawn.shape))
    spots = []
    for shift in (0, 1):
        where = [jax.random.randint(jax.random.fold_in(stream_key, axis), (), 0, length) for axis, length in enumerate(drawn.shape)]
        where[longest] = (where[longest] + shift) % drawn.shape[longest]
        spots.append(tuple(where))
    return drawn.at[spots[0]].set(low).at[spots[1]].set(top_value)


def block_scale(stream_key, extent, shards, low, largest):
    loudness = 1.0
    for axis_at, parts in shards:
        draws = jax.random.uniform(jax.random.fold_in(jax.random.fold_in(stream_key, 6), axis_at), (parts,), jnp.float32, low / len(shards), largest / len(shards))
        loudness = loudness * jnp.repeat(jnp.exp(draws), extent[axis_at] // parts).reshape((-1,) + (1,) * (len(extent) - 1 - axis_at))
    return loudness


def centred(key, shape, scale, most, cuts=(), kind=jnp.bfloat16):
    factor_of = block_scale(key, shape, cuts, -0.22, 0.18) if cuts else 1.0
    entries = jax.random.normal(key, shape, jnp.float32) * scale * factor_of
    return jnp.minimum(jnp.maximum(entries, -most), most).astype(kind)


def setup_inputs(seed: int = 0) -> dict:
    streams_of = jax.random.split(jax.random.key(seed), 10)
    return {
        "token_ids": draw_token_ids(jax.random.fold_in(streams_of[9], 71), 0),
        "lengths": touch_ends(jax.random.randint(streams_of[1], (B,), 1, L + 1), jax.random.fold_in(streams_of[1], 1), 1, L).astype(jnp.int32),
        "table": centred(streams_of[2], (VOCAB, D), 1.0, 6.0, ((0, 8), (1, 4))),
        "attn_gain": jnp.clip(1.0 + 0.18 * jax.random.normal(streams_of[3], (D,), jnp.float32), 0.1, 1.9),
        "w_qkv": draw_w_qkv(jax.random.fold_in(streams_of[9], 71), 0),
        "w_out": centred(streams_of[5], (D, D), D ** -0.5, 0.25),
        "mlp_gain": jnp.clip(1.0 + 0.18 * jax.random.normal(streams_of[6], (D,), jnp.float32), 0.1, 1.9),
        "w_in": centred(streams_of[7], (D, 2 * FF), D ** -0.5, 0.25),
        "w_down": centred(streams_of[8], (FF, D), FF ** -0.5, 0.125),
    }


def rms_norm(values_f32, gain):
    mean_sq = lax.optimization_barrier(jnp.mean(values_f32 * values_f32, axis=-1, keepdims=True))
    return values_f32 * lax.rsqrt(mean_sq + 1e-06) * gain

def layer(sequence, length, attn_gain, w_qkv, w_out, mlp_gain, w_in, w_down):
    residual = sequence.astype(jnp.float32)
    normed = rms_norm(residual, attn_gain).astype(jnp.bfloat16)
    projected = jnp.dot(normed, w_qkv, preferred_element_type=jnp.float32).astype(jnp.bfloat16)
    head_dim = D // HEADS
    queries = projected[:, :D].reshape(L, HEADS, head_dim).astype(jnp.float32)
    keys = projected[:, D:2 * D].reshape(L, HEADS, head_dim).astype(jnp.float32)
    values = projected[:, 2 * D:].reshape(L, HEADS, head_dim).astype(jnp.float32)
    scores = jnp.einsum('qhd,khd->hqk', queries, keys) * 0.125
    position = jnp.arange(L, dtype=jnp.int32)
    valid = (position[None, :] <= position[:, None]) & (position[None, :] < length)
    valid = valid[None, :, :]
    scores = jnp.where(valid, scores, -1e+30)
    row_max = lax.optimization_barrier(jnp.max(scores, axis=-1, keepdims=True))
    probs = jnp.where(valid, jnp.exp(scores - row_max), 0.0)
    total = lax.optimization_barrier(jnp.sum(probs, axis=-1))
    weights = probs.astype(jnp.bfloat16).astype(jnp.float32)
    summed = jnp.einsum('hqk,khd->hqd', weights, values) / total[..., None]
    attended = jnp.transpose(summed, (1, 0, 2)).reshape(L, D).astype(jnp.bfloat16)
    hidden = (residual + jnp.dot(attended, w_out, preferred_element_type=jnp.float32)).astype(jnp.bfloat16)
    hidden_f32 = hidden.astype(jnp.float32)
    normed_two = rms_norm(hidden_f32, mlp_gain).astype(jnp.bfloat16)
    gate_up = jnp.dot(normed_two, w_in, preferred_element_type=jnp.float32)
    act = (jax.nn.silu(gate_up[:, :FF]) * gate_up[:, FF:]).astype(jnp.bfloat16)
    return (hidden_f32 + jnp.dot(act, w_down, preferred_element_type=jnp.float32)).astype(jnp.bfloat16)

def reference(token_ids, lengths, table, attn_gain, w_qkv, w_out, mlp_gain, w_in, w_down):
    embedded = jnp.take(table, token_ids, axis=0)

    def one_history(pair):
        sequence, length = pair
        return layer(sequence, length, attn_gain, w_qkv, w_out, mlp_gain, w_in, w_down)
    return lax.map(one_history, (embedded, lengths))
```

```python
import functools

import jax
import jax.numpy as jnp
from jax import lax
from jax.experimental import pallas as pl
from jax.experimental.pallas import tpu as pltpu
from jax.sharding import PartitionSpec as P

HEADS = 8
LANES = 128
NEG = -1e30
SCORE_SCALE = 0.125 * 1.4426950408889634
MESH = pl.DeviceIdType.MESH
BF = jnp.bfloat16
F32 = jnp.float32


def rms_norm(values_f32, gain):
    mean_sq = jnp.mean(values_f32 * values_f32, axis=-1, keepdims=True)
    return values_f32 * lax.rsqrt(mean_sq + 1e-06) * gain


def layer_kernel(
    cols, lens_ref, e_ref, gain1, gain2, wq_h, wk_h, wv_h, wo_h, wi_h, wd_h, out_ref,
    ebuf, hbuf, hstage, wq, wk, wv, wo, wi, wd, qm, k_s, v_s, m_s, l_s, acc,
    send_sem, pass_sem, recv_sem, hsend_sem, hrecv_sem, own_sem, w_sem,
):
    me = lax.axis_index("cols")
    batch, full, width = e_ref.shape
    quarter = full // cols
    half = quarter // 2
    head_dim = LANES // 2
    group = cols // batch
    hist = me // group
    other = batch - 1 - hist
    inner = group - 1 + hist
    far_inner = group - 1 + other
    mate = hist * group + (group - 1 - lax.rem(me, group))
    is_inner = me == inner
    lo = jnp.where(is_inner, 0, 1)
    hi = cols - 1 - lo
    mate_hi = cols - 2 + lo

    def chunk(j):
        return pl.ds(pl.multiple_of(j * quarter, quarter), quarter)

    def far_copy(j):
        return pltpu.make_async_remote_copy(
            src_ref=e_ref.at[other, chunk(j)],
            dst_ref=ebuf.at[me, j],
            send_sem=send_sem.at[0, j],
            recv_sem=recv_sem.at[me, j],
            device_id={"cols": far_inner},
            device_id_type=MESH,
        )

    def mate_copy(j):
        return pltpu.make_async_remote_copy(
            src_ref=e_ref.at[hist, chunk(j)],
            dst_ref=ebuf.at[me, j],
            send_sem=send_sem.at[1, j],
            recv_sem=recv_sem.at[me, j],
            device_id={"cols": mate},
            device_id_type=MESH,
        )

    def pass_copy(s, j):
        return pltpu.make_async_remote_copy(
            src_ref=ebuf.at[s, j],
            dst_ref=ebuf.at[s, j],
            send_sem=pass_sem.at[s, j],
            recv_sem=recv_sem.at[s, j],
            device_id={"cols": mate},
            device_id_type=MESH,
        )

    def own_copy(j):
        return pltpu.make_async_copy(e_ref.at[hist, chunk(j)], ebuf.at[me, j], own_sem.at[j])

    def hidden_copy(slot, q):
        return pltpu.make_async_remote_copy(
            src_ref=hstage.at[slot],
            dst_ref=hbuf.at[hist],
            send_sem=hsend_sem.at[slot],
            recv_sem=hrecv_sem.at[hist],
            device_id={"cols": q},
            device_id_type=MESH,
        )

    barrier = pltpu.get_barrier_semaphore()
    for off in range(1, cols):
        pl.semaphore_signal(
            barrier, inc=1, device_id={"cols": lax.rem(me + off, cols)}, device_id_type=MESH
        )
    pl.semaphore_wait(barrier, cols - 1)

    for j in reversed(range(cols)):
        far_copy(j).start()

        @pl.when(j <= mate_hi)
        def _():
            mate_copy(j).start()

        @pl.when(j <= hi)
        def _():
            own_copy(j).start()

    loads = [
        pltpu.make_async_copy(src, dst, w_sem.at[i])
        for i, (src, dst) in enumerate(
            ((wq_h, wq), (wk_h, wk), (wv_h, wv), (wo_h, wo), (wi_h, wi), (wd_h, wd))
        )
    ]
    for load in loads:
        load.start()
    for load in loads[:3]:
        load.wait()

    dims_nt = (((1,), (1,)), ((), ()))
    length = lens_ref[hist]

    def embedded(j):
        parts = [ebuf[s, j] for s in range(cols)]
        return jnp.concatenate(parts, axis=1).astype(F32)

    def flash(slot, h, k_blk, v_t, q0, qn, causal):
        s = jnp.dot(k_blk, qm[slot, h, :, q0 : q0 + qn], preferred_element_type=F32)
        kn = k_blk.shape[0]
        if causal:
            key_pos = lax.broadcasted_iota(jnp.int32, (kn, qn), 0)
            query_pos = lax.broadcasted_iota(jnp.int32, (kn, qn), 1) + q0
            s = jnp.where(key_pos <= query_pos, s, NEG)
        m_old = m_s[slot, h, :, q0 : q0 + qn]
        m_new = jnp.maximum(m_old, jnp.max(s, axis=0, keepdims=True))
        probs = jnp.exp2(s - m_new)
        alpha = jnp.exp2(m_old - m_new)
        m_s[slot, h, :, q0 : q0 + qn] = m_new
        l_s[slot, h, :, q0 : q0 + qn] = l_s[slot, h, :, q0 : q0 + qn] * alpha + jnp.sum(
            probs, axis=0, keepdims=True
        )
        acc[slot, h, :, q0 : q0 + qn] = acc[slot, h, :, q0 : q0 + qn] * alpha + jnp.dot(
            v_t, probs.astype(BF), preferred_element_type=F32
        )

    def attend(slot, causal):
        def pair(p, carry):
            for side in range(2):
                h = 2 * p + side
                wide = pl.ds(pl.multiple_of(p * 2 * LANES, 2 * LANES), 2 * LANES)
                rows = pl.ds(pl.multiple_of(h * head_dim, head_dim), head_dim)
                if causal:
                    flash(slot, h, k_s[:half, wide], v_s[rows, :half], 0, half, True)
                    flash(slot, h, k_s[:, wide], v_s[rows, :], half, half, True)
                else:
                    flash(slot, h, k_s[:, wide], v_s[rows, :], 0, quarter, False)
            return carry

        lax.fori_loop(0, HEADS // 2, pair, 0)

    def finish(slot, q):
        att_t = (acc[slot] / l_s[slot]).reshape(HEADS * head_dim, quarter)
        attended = att_t.T.astype(BF)
        hidden = embedded(q) + jnp.dot(attended, wo[...], preferred_element_type=F32)
        hstage[slot] = hidden.astype(BF)
        hidden_copy(slot, q).start()

    def key_step(i, carry):
        j = hi - i
        own_copy(j).wait()
        for s in range(cols):

            @pl.when(me != s)
            def _():
                pass_copy(s, j).wait_recv()

            @pl.when(is_inner & (s // group == other) & (j <= cols - 2))
            def _():
                pass_copy(s, j).start()

        normed = rms_norm(embedded(j), gain1[...]).astype(BF)
        keys = jnp.dot(normed, wk[...], preferred_element_type=F32).astype(BF)
        row = lax.broadcasted_iota(jnp.int32, (quarter, LANES), 0)
        lane = lax.broadcasted_iota(jnp.int32, (quarter, LANES), 1)
        dead = (lane == 0) & (row >= length - j * quarter)
        bias = jnp.where(dead, NEG, 0.0).astype(BF)
        for p in range(HEADS // 2):
            k_s[:, 2 * p * LANES : (2 * p + 1) * LANES] = keys[:, p * LANES : (p + 1) * LANES]
            k_s[:, (2 * p + 1) * LANES : (2 * p + 2) * LANES] = bias
        v_s[...] = lax.dot_general(wv[...], normed, dims_nt, preferred_element_type=F32).astype(BF)

        @pl.when((j == hi) | (j == lo))
        def _():
            slot = jnp.where(j == hi, 0, 1)
            q_t = lax.dot_general(wq[...], normed, dims_nt, preferred_element_type=F32)
            q_t = (q_t * SCORE_SCALE).astype(BF)
            zero = jnp.zeros((head_dim, quarter), BF)
            one_row = lax.broadcasted_iota(jnp.int32, (LANES, quarter), 0) == 0
            one_row = jnp.where(one_row, 1.0, 0.0).astype(BF)
            for h in range(HEADS):
                mine = q_t[h * head_dim : (h + 1) * head_dim]
                pair = (mine, zero) if h % 2 == 0 else (zero, mine)
                qm[slot, h] = jnp.concatenate(pair + (one_row,), axis=0)
            m_s[slot] = jnp.full(m_s.shape[1:], NEG, F32)
            l_s[slot] = jnp.zeros(l_s.shape[1:], F32)
            acc[slot] = jnp.zeros(acc.shape[1:], F32)

        def query_step(slot, carry):
            q = jnp.where(slot == 0, hi, lo)

            @pl.when(j == q)
            def _():
                attend(slot, True)

            @pl.when(j < q)
            def _():
                attend(slot, False)

            @pl.when(j == 0)
            def _():
                finish(slot, q)

            return carry

        lax.fori_loop(0, 2, query_step, 0)
        return carry

    loads[3].wait()
    lax.fori_loop(0, hi + 1, key_step, 0)
    loads[4].wait()
    loads[5].wait()

    def mlp(i, carry):
        h = jnp.where(i == 0, hist, other)
        pltpu.make_async_remote_copy(
            src_ref=hbuf.at[h],
            dst_ref=hbuf.at[h],
            send_sem=hsend_sem.at[0],
            recv_sem=hrecv_sem.at[h],
            device_id={"cols": mate},
            device_id_type=MESH,
        ).wait_recv()
        hidden = hbuf[h].astype(F32)
        normed_two = rms_norm(hidden, gain2[...]).astype(BF)
        ff = wd.shape[0]
        tile = 512
        total = hidden
        for f in range(0, ff, tile):
            gate = jnp.dot(normed_two, wi[:, f : f + tile], preferred_element_type=F32)
            up = jnp.dot(normed_two, wi[:, ff + f : ff + f + tile], preferred_element_type=F32)
            act = (gate / (1.0 + jnp.exp(-gate)) * up).astype(BF)
            total = total + jnp.dot(act, wd[f : f + tile, :], preferred_element_type=F32)
        out_ref[h] = total.astype(BF)
        return carry

    lax.fori_loop(0, batch, mlp, 0)
    for j in reversed(range(cols)):
        far_copy(j).wait_send()

        @pl.when(j <= mate_hi)
        def _():
            mate_copy(j).wait_send()

        for s in range(cols):

            @pl.when(is_inner & (s // group == other) & (j <= cols - 2))
            def _():
                pass_copy(s, j).wait_send()

    hidden_copy(0, hi).wait_send()
    hidden_copy(1, lo).wait_send()


def layer_call(cols, lengths, emb, gain1, gain2, w_qkv, w_out, w_in, w_down):
    batch, full, width = emb.shape
    assert batch == 2 and cols == 2 * batch
    quarter = full // cols
    d = width * cols
    wq_t = w_qkv[:, :d].T
    wk = w_qkv[:, d : 2 * d]
    wv_t = w_qkv[:, 2 * d :].T
    any_spec = pl.BlockSpec(memory_space=pl.ANY)
    vmem = pl.BlockSpec(memory_space=pltpu.VMEM)
    smem = pl.BlockSpec(memory_space=pltpu.SMEM)
    weights = (wq_t, wk, wv_t, w_out, w_in, w_down)
    head_dim = d // HEADS
    return pl.pallas_call(
        functools.partial(layer_kernel, cols),
        out_shape=jax.ShapeDtypeStruct((batch, quarter, d), BF),
        in_specs=[smem, any_spec, vmem, vmem] + [any_spec] * 6,
        out_specs=vmem,
        scratch_shapes=[
            pltpu.VMEM((cols, cols, quarter, width), BF),
            pltpu.VMEM((batch, quarter, d), BF),
            pltpu.VMEM((2, quarter, d), BF),
        ]
        + [pltpu.VMEM(w.shape, BF) for w in weights]
        + [
            pltpu.VMEM((2, HEADS, 4 * head_dim, quarter), BF),
            pltpu.VMEM((quarter, 2 * d), BF),
            pltpu.VMEM((d, quarter), BF),
            pltpu.VMEM((2, HEADS, 1, quarter), F32),
            pltpu.VMEM((2, HEADS, 1, quarter), F32),
            pltpu.VMEM((2, HEADS, head_dim, quarter), F32),
            pltpu.SemaphoreType.DMA((2, cols)),
            pltpu.SemaphoreType.DMA((cols, cols)),
            pltpu.SemaphoreType.DMA((cols, cols)),
            pltpu.SemaphoreType.DMA((2,)),
            pltpu.SemaphoreType.DMA((batch,)),
            pltpu.SemaphoreType.DMA((cols,)),
            pltpu.SemaphoreType.DMA((6,)),
        ],
        compiler_params=pltpu.CompilerParams(
            collective_id=0, has_side_effects=True, vmem_limit_bytes=60 * 1024 * 1024
        ),
    )(lengths, emb, gain1.reshape(1, d), gain2.reshape(1, d), *weights)


def local(token_ids, lengths, table, attn_gain, w_qkv, w_out, mlp_gain, w_in, w_down):
    batch_dev, quarter = token_ids.shape
    col_count = lax.axis_size("cols")
    row_count = lax.axis_size("rows")
    full_len = quarter * col_count
    block_rows, col_width = table.shape
    own_ids = lax.all_gather(token_ids, "cols", axis=1, tiled=True)
    flat_ids = own_ids.reshape(-1)
    token_count = flat_ids.shape[0]
    capacity = -(-(8 * token_count // (3 * row_count)) // 16) * 16
    owner_block = flat_ids // block_rows
    offset = flat_ids - owner_block * block_rows
    onehot = (owner_block[:, None] == jnp.arange(row_count, dtype=jnp.int32)[None, :]).astype(
        jnp.int32
    )
    slot_rank = jnp.sum((jnp.cumsum(onehot, axis=0) - 1) * onehot, axis=1)
    slot_index = owner_block * capacity + slot_rank
    groups = -(-capacity // LANES)
    group_id = owner_block * groups + slot_rank // LANES
    left = (group_id[:, None] == jnp.arange(row_count * groups, dtype=jnp.int32)[None, :]).astype(BF)
    lane = slot_rank % LANES
    hit = lane[:, None] == jnp.arange(LANES, dtype=jnp.int32)[None, :]
    high = jnp.where(hit, (offset // LANES)[:, None], 0).astype(BF)
    low = jnp.where(hit, (offset % LANES)[:, None], 0).astype(BF)
    high = lax.dot_general(left, high, (((0,), (0,)), ((), ())), preferred_element_type=F32)
    low = lax.dot_general(left, low, (((0,), (0,)), ((), ())), preferred_element_type=F32)
    requests = (high * LANES + low).astype(jnp.int32)
    requests = requests.reshape(row_count, groups * LANES)[:, :capacity]
    asked = lax.all_to_all(requests, "rows", split_axis=0, concat_axis=0, tiled=True)
    looked = table.at[asked.reshape(-1)].get(mode="promise_in_bounds")
    returned = lax.all_to_all(looked, "rows", split_axis=0, concat_axis=0, tiled=True)
    emb = returned.at[slot_index].get(mode="promise_in_bounds")
    emb = emb.reshape(batch_dev, full_len, col_width)
    return layer_call(
        col_count, lengths, emb, attn_gain, mlp_gain, w_qkv, w_out, w_in, w_down
    )


def solution(mesh):
    in_specs = (P("rows", "cols"), P("rows"), P("rows", "cols"), P(), P(), P(), P(), P(), P())
    out_specs = P("rows", "cols", None)
    return jax.shard_map(local, mesh=mesh, in_specs=in_specs, out_specs=out_specs, check_vma=False)
```

```python
import functools

import jax
import jax.numpy as jnp
from jax import lax
from jax.experimental import pallas as pl
from jax.experimental.pallas import tpu as pltpu
from jax.sharding import PartitionSpec as P

HEADS = 8
LANES = 128
NEG = -1e30
SCORE_SCALE = 0.125 * 1.4426950408889634
MESH = pl.DeviceIdType.MESH
BF = jnp.bfloat16
F32 = jnp.float32


def rms_norm(values_f32, gain):
    mean_sq = jnp.mean(values_f32 * values_f32, axis=-1, keepdims=True)
    return values_f32 * lax.rsqrt(mean_sq + 1e-06) * gain


def layer_kernel(
    cols, lens_ref, e_ref, gain1, gain2, wq_h, wk_h, wv_h, wo_h, wi_h, wd_h, out_ref,
    ebuf, hbuf, hstage, wq, wk, wv, wo, wi, wd, qm, k_s, v_s, m_s, l_s, acc,
    send_sem, pass_sem, recv_sem, hsend_sem, hrecv_sem, own_sem, w_sem,
):
    me = lax.axis_index("cols")
    batch, full, width = e_ref.shape
    quarter = full // cols
    half = quarter // 2
    head_dim = LANES // 2
    group = cols // batch
    hist = me // group
    other = batch - 1 - hist
    inner = group - 1 + hist
    far_inner = group - 1 + other
    mate = hist * group + (group - 1 - lax.rem(me, group))
    is_inner = me == inner
    lo = jnp.where(is_inner, 0, 1)
    hi = cols - 1 - lo
    mate_hi = cols - 2 + lo

    def chunk(j):
        return pl.ds(pl.multiple_of(j * quarter, quarter), quarter)

    def far_copy(j):
        return pltpu.make_async_remote_copy(
            src_ref=e_ref.at[other, chunk(j)],
            dst_ref=ebuf.at[me, j],
            send_sem=send_sem.at[0, j],
            recv_sem=recv_sem.at[me, j],
            device_id={"cols": far_inner},
            device_id_type=MESH,
        )

    def mate_copy(j):
        return pltpu.make_async_remote_copy(
            src_ref=e_ref.at[hist, chunk(j)],
            dst_ref=ebuf.at[me, j],
            send_sem=send_sem.at[1, j],
            recv_sem=recv_sem.at[me, j],
            device_id={"cols": mate},
            device_id_type=MESH,
        )

    def pass_copy(s, j):
        return pltpu.make_async_remote_copy(
            src_ref=ebuf.at[s, j],
            dst_ref=ebuf.at[s, j],
            send_sem=pass_sem.at[s, j],
            recv_sem=recv_sem.at[s, j],
            device_id={"cols": mate},
            device_id_type=MESH,
        )

    def own_copy(j):
        return pltpu.make_async_copy(e_ref.at[hist, chunk(j)], ebuf.at[me, j], own_sem.at[j])

    def hidden_copy(slot, q):
        return pltpu.make_async_remote_copy(
            src_ref=hstage.at[slot],
            dst_ref=hbuf.at[hist],
            send_sem=hsend_sem.at[slot],
            recv_sem=hrecv_sem.at[hist],
            device_id={"cols": q},
            device_id_type=MESH,
        )

    barrier = pltpu.get_barrier_semaphore()
    for off in range(1, cols):
        pl.semaphore_signal(
            barrier, inc=1, device_id={"cols": lax.rem(me + off, cols)}, device_id_type=MESH
        )
    pl.semaphore_wait(barrier, cols - 1)

    for j in reversed(range(cols)):
        far_copy(j).start()

        @pl.when(j <= mate_hi)
        def _():
            mate_copy(j).start()

        @pl.when(j <= hi)
        def _():
            own_copy(j).start()

    loads = [
        pltpu.make_async_copy(src, dst, w_sem.at[i])
        for i, (src, dst) in enumerate(
            ((wq_h, wq), (wk_h, wk), (wv_h, wv), (wo_h, wo), (wi_h, wi), (wd_h, wd))
        )
    ]
    for load in loads:
        load.start()
    for load in loads[:3]:
        load.wait()

    dims_nt = (((1,), (1,)), ((), ()))
    length = lens_ref[hist]

    def embedded(j):
        parts = [ebuf[s, j] for s in range(cols)]
        return jnp.concatenate(parts, axis=1).astype(F32)

    def flash(slot, h, k_blk, v_t, q0, qn, causal):
        s = jnp.dot(k_blk, qm[slot, h, :, q0 : q0 + qn], preferred_element_type=F32)
        kn = k_blk.shape[0]
        if causal:
            key_pos = lax.broadcasted_iota(jnp.int32, (kn, qn), 0)
            query_pos = lax.broadcasted_iota(jnp.int32, (kn, qn), 1) + q0
            s = jnp.where(key_pos <= query_pos, s, NEG)
        m_old = m_s[slot, h, :, q0 : q0 + qn]
        m_new = jnp.maximum(m_old, jnp.max(s, axis=0, keepdims=True))
        probs = jnp.exp2(s - m_new)
        alpha = jnp.exp2(m_old - m_new)
        m_s[slot, h, :, q0 : q0 + qn] = m_new
        l_s[slot, h, :, q0 : q0 + qn] = l_s[slot, h, :, q0 : q0 + qn] * alpha + jnp.sum(
            probs, axis=0, keepdims=True
        )
        acc[slot, h, :, q0 : q0 + qn] = acc[slot, h, :, q0 : q0 + qn] * alpha + jnp.dot(
            v_t, probs.astype(BF), preferred_element_type=F32
        )

    def attend(slot, causal):
        def pair(p, carry):
            for side in range(2):
                h = 2 * p + side
                wide = pl.ds(pl.multiple_of(p * 2 * LANES, 2 * LANES), 2 * LANES)
                rows = pl.ds(pl.multiple_of(h * head_dim, head_dim), head_dim)
                if causal:
                    flash(slot, h, k_s[:half, wide], v_s[rows, :half], 0, half, True)
                    flash(slot, h, k_s[:, wide], v_s[rows, :], half, half, True)
                else:
                    flash(slot, h, k_s[:, wide], v_s[rows, :], 0, quarter, False)
            return carry

        lax.fori_loop(0, HEADS // 2, pair, 0)

    def finish(slot, q):
        att_t = (acc[slot] / l_s[slot]).reshape(HEADS * head_dim, quarter)
        attended = att_t.T.astype(BF)
        hidden = embedded(q) + jnp.dot(attended, wo[...], preferred_element_type=F32)
        hstage[slot] = hidden.astype(BF)
        hidden_copy(slot, q).start()

    def key_step(i, carry):
        j = hi - i
        own_copy(j).wait()
        for s in range(cols):

            @pl.when(me != s)
            def _():
                pass_copy(s, j).wait_recv()

            @pl.when(is_inner & (s // group == other) & (j <= cols - 2))
            def _():
                pass_copy(s, j).start()

        normed = rms_norm(embedded(j), gain1[...]).astype(BF)
        keys = jnp.dot(normed, wk[...], preferred_element_type=F32).astype(BF)
        row = lax.broadcasted_iota(jnp.int32, (quarter, LANES), 0)
        lane = lax.broadcasted_iota(jnp.int32, (quarter, LANES), 1)
        dead = (lane == 0) & (row >= length - j * quarter)
        bias = jnp.where(dead, NEG, 0.0).astype(BF)
        for p in range(HEADS // 2):
            k_s[:, 2 * p * LANES : (2 * p + 1) * LANES] = keys[:, p * LANES : (p + 1) * LANES]
            k_s[:, (2 * p + 1) * LANES : (2 * p + 2) * LANES] = bias
        v_s[...] = lax.dot_general(wv[...], normed, dims_nt, preferred_element_type=F32).astype(BF)

        @pl.when((j == hi) | (j == lo))
        def _():
            slot = jnp.where(j == hi, 0, 1)
            q_t = lax.dot_general(wq[...], normed, dims_nt, preferred_element_type=F32)
            q_t = (q_t * SCORE_SCALE).astype(BF)
            zero = jnp.zeros((head_dim, quarter), BF)
            one_row = lax.broadcasted_iota(jnp.int32, (LANES, quarter), 0) == 0
            one_row = jnp.where(one_row, 1.0, 0.0).astype(BF)
            for h in range(HEADS):
                mine = q_t[h * head_dim : (h + 1) * head_dim]
                pair = (mine, zero) if h % 2 == 0 else (zero, mine)
                qm[slot, h] = jnp.concatenate(pair + (one_row,), axis=0)
            m_s[slot] = jnp.full(m_s.shape[1:], NEG, F32)
            l_s[slot] = jnp.zeros(l_s.shape[1:], F32)
            acc[slot] = jnp.zeros(acc.shape[1:], F32)

        def query_step(slot, carry):
            q = jnp.where(slot == 0, hi, lo)

            @pl.when(j == q)
            def _():
                attend(slot, True)

            @pl.when(j < q)
            def _():
                attend(slot, False)

            @pl.when(j == 0)
            def _():
                finish(slot, q)

            return carry

        lax.fori_loop(0, 2, query_step, 0)
        return carry

    loads[3].wait()
    lax.fori_loop(0, hi + 1, key_step, 0)
    loads[4].wait()
    loads[5].wait()

    def mlp(i, carry):
        h = jnp.where(i == 0, hist, other)
        pltpu.make_async_remote_copy(
            src_ref=hbuf.at[h],
            dst_ref=hbuf.at[h],
            send_sem=hsend_sem.at[0],
            recv_sem=hrecv_sem.at[h],
            device_id={"cols": mate},
            device_id_type=MESH,
        ).wait_recv()
        hidden = hbuf[h].astype(F32)
        normed_two = rms_norm(hidden, gain2[...]).astype(BF)
        ff = wd.shape[0]
        tile = 512
        total = hidden
        for f in range(0, ff, tile):
            gate = jnp.dot(normed_two, wi[:, f : f + tile], preferred_element_type=F32)
            up = jnp.dot(normed_two, wi[:, ff + f : ff + f + tile], preferred_element_type=F32)
            act = (gate / (1.0 + jnp.exp(-gate)) * up).astype(BF)
            total = total + jnp.dot(act, wd[f : f + tile, :], preferred_element_type=F32)
        out_ref[h] = total.astype(BF)
        return carry

    lax.fori_loop(0, batch, mlp, 0)
    for j in reversed(range(cols)):
        far_copy(j).wait_send()

        @pl.when(j <= mate_hi)
        def _():
            mate_copy(j).wait_send()

        for s in range(cols):

            @pl.when(is_inner & (s // group == other) & (j <= cols - 2))
            def _():
                pass_copy(s, j).wait_send()

    hidden_copy(0, hi).wait_send()
    hidden_copy(1, lo).wait_send()


def layer_call(cols, lengths, emb, gain1, gain2, w_qkv, w_out, w_in, w_down):
    batch, full, width = emb.shape
    assert batch == 2 and cols == 2 * batch
    quarter = full // cols
    d = width * cols
    wq_t = w_qkv[:, :d].T
    wk = w_qkv[:, d : 2 * d]
    wv_t = w_qkv[:, 2 * d :].T
    any_spec = pl.BlockSpec(memory_space=pl.ANY)
    vmem = pl.BlockSpec(memory_space=pltpu.VMEM)
    smem = pl.BlockSpec(memory_space=pltpu.SMEM)
    weights = (wq_t, wk, wv_t, w_out, w_in, w_down)
    head_dim = d // HEADS
    return pl.pallas_call(
        functools.partial(layer_kernel, cols),
        out_shape=jax.ShapeDtypeStruct((batch, quarter, d), BF),
        in_specs=[smem, any_spec, vmem, vmem] + [any_spec] * 6,
        out_specs=vmem,
        scratch_shapes=[
            pltpu.VMEM((cols, cols, quarter, width), BF),
            pltpu.VMEM((batch, quarter, d), BF),
            pltpu.VMEM((2, quarter, d), BF),
        ]
        + [pltpu.VMEM(w.shape, BF) for w in weights]
        + [
            pltpu.VMEM((2, HEADS, 4 * head_dim, quarter), BF),
            pltpu.VMEM((quarter, 2 * d), BF),
            pltpu.VMEM((d, quarter), BF),
            pltpu.VMEM((2, HEADS, 1, quarter), F32),
            pltpu.VMEM((2, HEADS, 1, quarter), F32),
            pltpu.VMEM((2, HEADS, head_dim, quarter), F32),
            pltpu.SemaphoreType.DMA((2, cols)),
            pltpu.SemaphoreType.DMA((cols, cols)),
            pltpu.SemaphoreType.DMA((cols, cols)),
            pltpu.SemaphoreType.DMA((2,)),
            pltpu.SemaphoreType.DMA((batch,)),
            pltpu.SemaphoreType.DMA((cols,)),
            pltpu.SemaphoreType.DMA((6,)),
        ],
        compiler_params=pltpu.CompilerParams(
            collective_id=0, has_side_effects=True, vmem_limit_bytes=60 * 1024 * 1024
        ),
    )(lengths, emb, gain1.reshape(1, d), gain2.reshape(1, d), *weights)


def fetch_kernel(
    rows, cols, cap, ids_ref, table_ref, ret_ref, slot_ref,
    ids_all, ids_s, left, right, req, asked, asked_s, tab, wide_tab, stage, outbox,
    ids_send, ids_recv, req_send, req_recv, row_send, row_recv, tab_sem, smem_sem, own_sem,
):
    mc = lax.axis_index("cols")
    mr = lax.axis_index("rows")
    batch, quarter = ids_ref.shape
    block_rows, width = table_ref.shape
    tiles = quarter // LANES
    lines = ids_s.shape[0]
    tokens = lines * LANES
    groups = req.shape[1]
    pieces = tab_sem.shape[0]
    piece = block_rows // pieces
    shift = block_rows.bit_length() - 1

    def tab_copy(i):
        part = pl.ds(i * piece, piece)
        return pltpu.make_async_copy(table_ref.at[part], tab.at[part], tab_sem.at[i])

    for i in range(pieces):
        tab_copy(i).start()

    def ids_copy(c):
        return pltpu.make_async_remote_copy(
            src_ref=ids_ref,
            dst_ref=ids_all.at[mc],
            send_sem=ids_send.at[c],
            recv_sem=ids_recv.at[mc],
            device_id={"cols": c},
            device_id_type=MESH,
        )

    def ids_arrival(c):
        return pltpu.make_async_remote_copy(
            src_ref=ids_ref,
            dst_ref=ids_all.at[c],
            send_sem=ids_send.at[c],
            recv_sem=ids_recv.at[c],
            device_id={"cols": c},
            device_id_type=MESH,
        )

    def req_copy(r):
        return pltpu.make_async_remote_copy(
            src_ref=req.at[r],
            dst_ref=asked.at[mr],
            send_sem=req_send.at[r],
            recv_sem=req_recv.at[mr],
            device_id={"rows": r},
            device_id_type=MESH,
        )

    def req_arrival(r):
        return pltpu.make_async_remote_copy(
            src_ref=req.at[r],
            dst_ref=asked.at[r],
            send_sem=req_send.at[r],
            recv_sem=req_recv.at[r],
            device_id={"rows": r},
            device_id_type=MESH,
        )

    def row_copy(r):
        return pltpu.make_async_remote_copy(
            src_ref=outbox.at[r],
            dst_ref=ret_ref.at[mr],
            send_sem=row_send.at[r],
            recv_sem=row_recv.at[mr],
            device_id={"rows": r},
            device_id_type=MESH,
        )

    def row_arrival(r):
        return pltpu.make_async_remote_copy(
            src_ref=outbox.at[r],
            dst_ref=ret_ref.at[r],
            send_sem=row_send.at[r],
            recv_sem=row_recv.at[r],
            device_id={"rows": r},
            device_id_type=MESH,
        )

    barrier = pltpu.get_barrier_semaphore()
    for off in range(1, cols):
        pl.semaphore_signal(
            barrier, inc=1, device_id={"cols": lax.rem(mc + off, cols)}, device_id_type=MESH
        )
    for off in range(1, rows):
        pl.semaphore_signal(
            barrier, inc=1, device_id={"rows": lax.rem(mr + off, rows)}, device_id_type=MESH
        )
    pl.semaphore_wait(barrier, cols - 1 + rows - 1)

    for off in range(1, cols):
        ids_copy(lax.rem(mc + off, cols)).start()
    ids_all[mc] = ids_ref[...]

    step = 512
    for i in range(pieces):
        tab_copy(i).wait()

        def widen(k, carry):
            part = pl.ds(pl.multiple_of(i * piece + k * step, step), step)
            wide_tab[part, :] = tab[part, :].astype(F32)
            return carry

        lax.fori_loop(0, piece // step, widen, 0)

    for off in range(1, cols):
        ids_arrival(lax.rem(mc + off, cols)).wait_recv()
    for c in range(cols):
        for b in range(batch):
            for k in range(tiles):
                line = (c * batch + b) * tiles + k
                ids_s[line : line + 1, :] = ids_all[c, b : b + 1, k * LANES : (k + 1) * LANES]
    ids = ids_s[...]
    owner = lax.shift_right_logical(ids, shift)
    offset = ids - owner * block_rows

    src_lane = lax.broadcasted_iota(jnp.int32, (LANES, 2 * LANES), 0)
    dst_lane = lax.broadcasted_iota(jnp.int32, (LANES, 2 * LANES), 1)
    before = jnp.where(src_lane < dst_lane, 1.0, 0.0).astype(BF)
    line_a = lax.broadcasted_iota(jnp.int32, (lines, lines), 0)
    line_b = lax.broadcasted_iota(jnp.int32, (lines, lines), 1)
    above = jnp.where(line_b < line_a, 1.0, 0.0).astype(BF)
    rank = jnp.zeros((lines, LANES), F32)
    for r in range(rows):
        mine = owner == r
        counts = jnp.dot(
            jnp.where(mine, 1.0, 0.0).astype(BF), before, preferred_element_type=F32
        )
        earlier = jnp.dot(above, counts[:, LANES:].astype(BF), preferred_element_type=F32)
        rank = rank + jnp.where(mine, counts[:, :LANES] + earlier, 0.0)
    rank = rank.astype(jnp.int32)
    slot_ref[...] = owner * cap + rank
    group = owner * groups + lax.shift_right_logical(rank, 7)
    lane = rank - lax.shift_right_logical(rank, 7) * LANES
    high = lax.shift_right_logical(offset, 7)
    low = (offset - high * LANES).astype(F32)
    high = high.astype(F32)
    group_iota = lax.broadcasted_iota(jnp.int32, (rows * groups, LANES), 0)
    lane_iota = lax.broadcasted_iota(jnp.int32, (LANES, LANES), 0)
    for k in range(lines):
        part = slice(k * LANES, (k + 1) * LANES)
        line = slice(k, k + 1)
        left[:, part] = jnp.where(group[line] == group_iota, 1.0, 0.0).astype(BF)
        hit = lane[line] == lane_iota
        right[:LANES, part] = jnp.where(hit, high[line], 0.0).astype(BF)
        right[LANES:, part] = jnp.where(hit, low[line], 0.0).astype(BF)
    found = lax.dot_general(
        left[...], right[...], (((1,), (1,)), ((), ())), preferred_element_type=F32
    )
    found = (found[:, :LANES] * LANES + found[:, LANES:]).astype(jnp.int32)
    found = jnp.minimum(jnp.maximum(found, 0), block_rows - 1)
    req[...] = found.reshape(rows, groups, LANES)

    def over_rows(act):
        def body(i, carry):
            act(lax.rem(mr + i + 1, rows))
            return carry

        lax.fori_loop(0, rows - 1, body, 0)

    over_rows(lambda r: req_copy(r).start())
    asked[mr] = req[mr]
    over_rows(lambda r: req_arrival(r).wait_recv())
    to_smem = pltpu.make_async_copy(asked, asked_s, smem_sem)
    to_smem.start()
    to_smem.wait()

    unroll = stage.shape[0]
    own = pltpu.make_async_copy(outbox.at[mr], ret_ref.at[mr], own_sem)

    def serve(i, carry):
        dist = (i + 1) // 2
        off = rows // 2 + dist * (1 - 2 * lax.rem(i, 2))
        r = lax.rem(mr + off, rows)

        def some(k, carry):
            base = k * unroll
            g = base // LANES
            first = base - g * LANES
            for u in range(unroll):
                at = asked_s[r, g, first + u]
                stage[u : u + 1, :] = wide_tab[pl.ds(at, 1), :]
            outbox[r, pl.ds(pl.multiple_of(base, unroll), unroll), :] = stage[...].astype(BF)
            return carry

        lax.fori_loop(0, cap // unroll, some, 0)

        @pl.when(i < rows - 1)
        def _():
            row_copy(r).start()

        return carry

    lax.fori_loop(0, rows, serve, 0)
    own.start()
    own.wait()
    over_rows(lambda r: row_arrival(r).wait_recv())
    for off in range(1, cols):
        ids_copy(lax.rem(mc + off, cols)).wait_send()
    over_rows(lambda r: req_copy(r).wait_send())
    over_rows(lambda r: row_copy(r).wait_send())


def fetch_call(rows, cols, cap, token_ids, table):
    batch, quarter = token_ids.shape
    tokens = batch * quarter * cols
    lines = tokens // LANES
    block_rows, width = table.shape
    assert block_rows & (block_rows - 1) == 0 and rows % 2 == 0
    groups = -(-cap // (8 * LANES)) * 8
    any_spec = pl.BlockSpec(memory_space=pl.ANY)
    vmem = pl.BlockSpec(memory_space=pltpu.VMEM)
    dma = pltpu.SemaphoreType.DMA
    return pl.pallas_call(
        functools.partial(fetch_kernel, rows, cols, cap),
        out_shape=(
            jax.ShapeDtypeStruct((rows, cap, width), BF),
            jax.ShapeDtypeStruct((lines, LANES), jnp.int32),
        ),
        in_specs=[vmem, any_spec],
        out_specs=(any_spec, vmem),
        scratch_shapes=[
            pltpu.VMEM((cols, batch, quarter), jnp.int32),
            pltpu.VMEM((lines, LANES), jnp.int32),
            pltpu.VMEM((rows * groups, tokens), BF),
            pltpu.VMEM((2 * LANES, tokens), BF),
            pltpu.VMEM((rows, groups, LANES), jnp.int32),
            pltpu.VMEM((rows, groups, LANES), jnp.int32),
            pltpu.SMEM((rows, groups, LANES), jnp.int32),
            pltpu.VMEM((block_rows, width), BF),
            pltpu.VMEM((block_rows, width), F32),
            pltpu.VMEM((32, width), F32),
            pltpu.VMEM((rows, cap, width), BF),
            dma((cols,)),
            dma((cols,)),
            dma((rows,)),
            dma((rows,)),
            dma((rows,)),
            dma((rows,)),
            dma((4,)),
            dma,
            dma,
        ],
        compiler_params=pltpu.CompilerParams(
            collective_id=1, has_side_effects=True, vmem_limit_bytes=60 * 1024 * 1024
        ),
    )(token_ids, table)


def local(token_ids, lengths, table, attn_gain, w_qkv, w_out, mlp_gain, w_in, w_down):
    batch_dev, quarter = token_ids.shape
    col_count = lax.axis_size("cols")
    row_count = lax.axis_size("rows")
    full_len = quarter * col_count
    token_count = batch_dev * full_len
    capacity = -(-(8 * token_count // (3 * row_count)) // 32) * 32
    returned, slots = fetch_call(row_count, col_count, capacity, token_ids, table)
    slots = slots.reshape(col_count, batch_dev, quarter).transpose(1, 0, 2).reshape(-1)
    flat = returned.reshape(row_count * capacity, -1)
    emb = flat.at[slots].get(mode="promise_in_bounds")
    emb = emb.reshape(batch_dev, full_len, -1)
    return layer_call(
        col_count, lengths, emb, attn_gain, mlp_gain, w_qkv, w_out, w_in, w_down
    )


def solution(mesh):
    in_specs = (P("rows", "cols"), P("rows"), P("rows", "cols"), P(), P(), P(), P(), P(), P())
    out_specs = P("rows", "cols", None)
    return jax.shard_map(local, mesh=mesh, in_specs=in_specs, out_specs=out_specs, check_vma=False)
```

```python
import functools

import jax
import jax.numpy as jnp
from jax import lax
from jax.experimental import pallas as pl
from jax.experimental.pallas import tpu as pltpu
from jax.sharding import PartitionSpec as P

HEADS = 8
LANES = 128
NEG = -1e30
SCORE_SCALE = 0.125 * 1.4426950408889634
MESH = pl.DeviceIdType.MESH
BF = jnp.bfloat16
F32 = jnp.float32


def rms_norm(values_f32, gain):
    mean_sq = jnp.mean(values_f32 * values_f32, axis=-1, keepdims=True)
    return values_f32 * lax.rsqrt(mean_sq + 1e-06) * gain


def layer_kernel(
    cols, batch, lens_ref, slots_ref, raw_ref, gain1, gain2, wq_h, wk_h, wv_h, wo_h, wi_h, wd_h,
    out_ref, raw, wide, stage, ebox, ebuf, hbuf, hstage, wq, wk, wv, wo, wi, wd, qm, k_s, v_s,
    m_s, l_s, acc, raw_sem, send_sem, pass_sem, recv_sem, hsend_sem, hrecv_sem, w_sem,
):
    me = lax.axis_index("cols")
    rows, cap, width = raw_ref.shape
    quarter = ebox.shape[1]
    half = quarter // 2
    head_dim = LANES // 2
    group = cols // batch
    hist = me // group
    other = batch - 1 - hist
    inner = group - 1 + hist
    far_inner = group - 1 + other
    mate = hist * group + (group - 1 - lax.rem(me, group))
    is_inner = me == inner
    falling = hist == 0
    hi = jnp.where(is_inner, cols - 2, cols - 1)
    mate_hi = jnp.where(is_inner, cols - 1, cols - 2)
    q_sent = jnp.where(falling, hi, cols - 1 - hi)
    q_kept = cols - 1 - q_sent

    def order(h, t):
        return jnp.where(h == 0, cols - 1 - t, t)

    def raw_copy(r):
        return pltpu.make_async_copy(
            raw_ref.at[r], raw.at[pl.ds(pl.multiple_of(r * cap, 16), cap)], raw_sem.at[r]
        )

    def far_copy(j):
        return pltpu.make_async_remote_copy(
            src_ref=ebox.at[j],
            dst_ref=ebuf.at[me, j],
            send_sem=send_sem.at[0, j],
            recv_sem=recv_sem.at[me, j],
            device_id={"cols": far_inner},
            device_id_type=MESH,
        )

    def mate_copy(j):
        return pltpu.make_async_remote_copy(
            src_ref=ebuf.at[me, j],
            dst_ref=ebuf.at[me, j],
            send_sem=send_sem.at[1, j],
            recv_sem=recv_sem.at[me, j],
            device_id={"cols": mate},
            device_id_type=MESH,
        )

    def pass_copy(s, j):
        return pltpu.make_async_remote_copy(
            src_ref=ebuf.at[s, j],
            dst_ref=ebuf.at[s, j],
            send_sem=pass_sem.at[s, j],
            recv_sem=recv_sem.at[s, j],
            device_id={"cols": mate},
            device_id_type=MESH,
        )

    def hidden_copy():
        return pltpu.make_async_remote_copy(
            src_ref=hstage,
            dst_ref=hbuf.at[hist],
            send_sem=hsend_sem,
            recv_sem=hrecv_sem,
            device_id={"cols": q_sent},
            device_id_type=MESH,
        )

    def start_raw(r, carry):
        raw_copy(r).start()
        return carry

    lax.fori_loop(0, rows, start_raw, 0)
    loads = [
        pltpu.make_async_copy(src, dst, w_sem.at[i])
        for i, (src, dst) in enumerate(
            ((wq_h, wq), (wk_h, wk), (wv_h, wv), (wo_h, wo), (wi_h, wi), (wd_h, wd))
        )
    ]
    for load in loads:
        load.start()

    barrier = pltpu.get_barrier_semaphore()
    for off in range(1, cols):
        pl.semaphore_signal(
            barrier, inc=1, device_id={"cols": lax.rem(me + off, cols)}, device_id_type=MESH
        )

    def widen(r, carry):
        raw_copy(r).wait()
        part = pl.ds(pl.multiple_of(r * cap, 16), cap)
        wide[part, :] = raw[part, :].astype(F32)
        return carry

    lax.fori_loop(0, rows, widen, 0)
    pl.semaphore_wait(barrier, cols - 1)

    tiles = quarter // LANES

    def pick(t, carry):
        for side in range(2):
            h = other if side == 0 else hist
            j = order(h, t)
            line = (j * batch + h) * tiles
            for k in range(tiles):
                for u in range(LANES):
                    stage[u : u + 1, :] = wide[pl.ds(slots_ref[line + k, u], 1), :]
                part = slice(k * LANES, (k + 1) * LANES)
                if side == 0:
                    ebox[j, part, :] = stage[...].astype(BF)
                else:
                    ebuf[me, j, part, :] = stage[...].astype(BF)
            if side == 0:
                far_copy(j).start()
            else:

                @pl.when(j <= mate_hi)
                def _():
                    mate_copy(j).start()

        return carry

    lax.fori_loop(0, cols, pick, 0)
    for load in loads:
        load.wait()

    dims_nt = (((1,), (1,)), ((), ()))
    length = lens_ref[hist]

    def embedded(j):
        parts = [ebuf[s, j] for s in range(cols)]
        return jnp.concatenate(parts, axis=1).astype(F32)

    def flash(slot, h, k_blk, v_t, q0, qn, causal):
        s = jnp.dot(k_blk, qm[slot, h, :, q0 : q0 + qn], preferred_element_type=F32)
        kn = k_blk.shape[0]
        if causal:
            key_pos = lax.broadcasted_iota(jnp.int32, (kn, qn), 0)
            query_pos = lax.broadcasted_iota(jnp.int32, (kn, qn), 1) + q0
            s = jnp.where(key_pos <= query_pos, s, NEG)
        m_old = m_s[slot, h, :, q0 : q0 + qn]
        m_new = jnp.maximum(m_old, jnp.max(s, axis=0, keepdims=True))
        probs = jnp.exp2(s - m_new)
        alpha = jnp.exp2(m_old - m_new)
        m_s[slot, h, :, q0 : q0 + qn] = m_new
        l_s[slot, h, :, q0 : q0 + qn] = l_s[slot, h, :, q0 : q0 + qn] * alpha + jnp.sum(
            probs, axis=0, keepdims=True
        )
        acc[slot, h, :, q0 : q0 + qn] = acc[slot, h, :, q0 : q0 + qn] * alpha + jnp.dot(
            v_t, probs.astype(BF), preferred_element_type=F32
        )

    def attend(slot, j, causal):
        def pair(p, carry):
            for side in range(2):
                h = 2 * p + side
                wide_p = pl.ds(pl.multiple_of(p * 2 * LANES, 2 * LANES), 2 * LANES)
                part = pl.ds(pl.multiple_of(h * head_dim, head_dim), head_dim)
                if causal:
                    flash(slot, h, k_s[j, :half, wide_p], v_s[j, part, :half], 0, half, True)
                    flash(slot, h, k_s[j, :, wide_p], v_s[j, part, :], half, half, True)
                else:
                    flash(slot, h, k_s[j, :, wide_p], v_s[j, part, :], 0, quarter, False)
            return carry

        lax.fori_loop(0, HEADS // 2, pair, 0)

    def arrive(j):
        for s in range(cols):
            far = s // group == other

            @pl.when(far | ((s != me) & (j <= hi)))
            def _():
                pass_copy(s, j).wait_recv()

            @pl.when(is_inner & far)
            def _():
                pass_copy(s, j).start()

    def project(j):
        normed = rms_norm(embedded(j), gain1[...]).astype(BF)
        keys = jnp.dot(normed, wk[...], preferred_element_type=F32).astype(BF)
        row = lax.broadcasted_iota(jnp.int32, (quarter, LANES), 0)
        lane = lax.broadcasted_iota(jnp.int32, (quarter, LANES), 1)
        dead = (lane == 0) & (row >= length - j * quarter)
        bias = jnp.where(dead, NEG, 0.0).astype(BF)
        for p in range(HEADS // 2):
            k_s[j, :, 2 * p * LANES : (2 * p + 1) * LANES] = keys[:, p * LANES : (p + 1) * LANES]
            k_s[j, :, (2 * p + 1) * LANES : (2 * p + 2) * LANES] = bias
        v_s[j] = lax.dot_general(wv[...], normed, dims_nt, preferred_element_type=F32).astype(BF)

        @pl.when((j == q_sent) | (j == q_kept))
        def _():
            slot = jnp.where(j == q_sent, 0, 1)
            q_t = lax.dot_general(wq[...], normed, dims_nt, preferred_element_type=F32)
            q_t = (q_t * SCORE_SCALE).astype(BF)
            zero = jnp.zeros((head_dim, quarter), BF)
            one_row = lax.broadcasted_iota(jnp.int32, (LANES, quarter), 0) == 0
            one_row = jnp.where(one_row, 1.0, 0.0).astype(BF)
            for h in range(HEADS):
                mine = q_t[h * head_dim : (h + 1) * head_dim]
                pair = (mine, zero) if h % 2 == 0 else (zero, mine)
                qm[slot, h] = jnp.concatenate(pair + (one_row,), axis=0)
            m_s[slot] = jnp.full(m_s.shape[1:], NEG, F32)
            l_s[slot] = jnp.zeros(l_s.shape[1:], F32)
            acc[slot] = jnp.zeros(acc.shape[1:], F32)

    def step(t, carry):
        last = t == cols
        j = order(hist, jnp.minimum(t, cols - 1))

        @pl.when(t < cols)
        def _():
            arrive(j)

            @pl.when(j <= hi)
            def _():
                project(j)

        slot = jnp.where(last, 1, 0)
        q = jnp.where(last, q_kept, q_sent)
        whole = last | ((hist > 0) & (j == q_sent))
        piece = (hist == 0) & (j <= q_sent) & (t < cols)
        count = jnp.where(whole, q + 1, jnp.where(piece, 1, 0))
        first = jnp.where(whole, q, j)

        def unit(i, carry):
            key = first - i

            @pl.when(key == q)
            def _():
                attend(slot, key, True)

            @pl.when(key < q)
            def _():
                attend(slot, key, False)

            @pl.when(key == 0)
            def _():
                att_t = (acc[slot] / l_s[slot]).reshape(HEADS * head_dim, quarter)
                attended = att_t.T.astype(BF)
                hidden = embedded(q) + jnp.dot(attended, wo[...], preferred_element_type=F32)
                hidden = hidden.astype(BF)

                @pl.when(last)
                def _():
                    hbuf[hist] = hidden

                @pl.when(t < cols)
                def _():
                    hstage[...] = hidden
                    hidden_copy().start()

            return carry

        lax.fori_loop(0, count, unit, 0)
        return carry

    lax.fori_loop(0, cols + 1, step, 0)

    def mlp(i, carry):
        h = jnp.where(i == 0, hist, other)

        @pl.when(i > 0)
        def _():
            hidden_copy().wait_recv()

        hidden = hbuf[h].astype(F32)
        normed_two = rms_norm(hidden, gain2[...]).astype(BF)
        ff = wd.shape[0]
        tile = 512
        total = hidden
        for f in range(0, ff, tile):
            gate = jnp.dot(normed_two, wi[:, f : f + tile], preferred_element_type=F32)
            up = jnp.dot(normed_two, wi[:, ff + f : ff + f + tile], preferred_element_type=F32)
            act = (gate / (1.0 + jnp.exp(-gate)) * up).astype(BF)
            total = total + jnp.dot(act, wd[f : f + tile, :], preferred_element_type=F32)
        out_ref[h] = total.astype(BF)
        return carry

    lax.fori_loop(0, batch, mlp, 0)
    for j in range(cols):
        far_copy(j).wait_send()

        @pl.when(j <= mate_hi)
        def _():
            mate_copy(j).wait_send()

        for s in range(cols):

            @pl.when(is_inner & (s // group == other))
            def _():
                pass_copy(s, j).wait_send()

    hidden_copy().wait_send()


def layer_call(cols, batch, lengths, slots, returned, gain1, gain2, w_qkv, w_out, w_in, w_down):
    rows, cap, width = returned.shape
    assert batch == 2 and cols == 2 * batch
    quarter = slots.size // (batch * cols)
    d = width * cols
    wq_t = w_qkv[:, :d].T
    wk = w_qkv[:, d : 2 * d]
    wv_t = w_qkv[:, 2 * d :].T
    any_spec = pl.BlockSpec(memory_space=pl.ANY)
    vmem = pl.BlockSpec(memory_space=pltpu.VMEM)
    smem = pl.BlockSpec(memory_space=pltpu.SMEM)
    weights = (wq_t, wk, wv_t, w_out, w_in, w_down)
    head_dim = d // HEADS
    dma = pltpu.SemaphoreType.DMA
    return pl.pallas_call(
        functools.partial(layer_kernel, cols, batch),
        out_shape=jax.ShapeDtypeStruct((batch, quarter, d), BF),
        in_specs=[smem, smem, any_spec, vmem, vmem] + [any_spec] * 6,
        out_specs=vmem,
        scratch_shapes=[
            pltpu.VMEM((rows * cap, width), BF),
            pltpu.VMEM((rows * cap, width), F32),
            pltpu.VMEM((LANES, width), F32),
            pltpu.VMEM((cols, quarter, width), BF),
            pltpu.VMEM((cols, cols, quarter, width), BF),
            pltpu.VMEM((batch, quarter, d), BF),
            pltpu.VMEM((quarter, d), BF),
        ]
        + [pltpu.VMEM(w.shape, BF) for w in weights]
        + [
            pltpu.VMEM((2, HEADS, 4 * head_dim, quarter), BF),
            pltpu.VMEM((cols, quarter, 2 * d), BF),
            pltpu.VMEM((cols, d, quarter), BF),
            pltpu.VMEM((2, HEADS, 1, quarter), F32),
            pltpu.VMEM((2, HEADS, 1, quarter), F32),
            pltpu.VMEM((2, HEADS, head_dim, quarter), F32),
            dma((rows,)),
            dma((2, cols)),
            dma((cols, cols)),
            dma((cols, cols)),
            dma,
            dma,
            dma((6,)),
        ],
        compiler_params=pltpu.CompilerParams(
            collective_id=0, has_side_effects=True, vmem_limit_bytes=60 * 1024 * 1024
        ),
    )(lengths, slots, returned, gain1.reshape(1, d), gain2.reshape(1, d), *weights)


def fetch_kernel(
    rows, cols, cap, ids_ref, table_ref, ret_ref, slot_ref,
    ids_all, ids_s, left, right, req, asked, asked_s, tab, wide_tab, stage, outbox,
    ids_send, ids_recv, req_send, req_recv, row_send, row_recv, tab_sem, smem_sem, own_sem,
):
    mc = lax.axis_index("cols")
    mr = lax.axis_index("rows")
    batch, quarter = ids_ref.shape
    block_rows, width = table_ref.shape
    tiles = quarter // LANES
    lines = ids_s.shape[0]
    tokens = lines * LANES
    groups = req.shape[1]
    pieces = tab_sem.shape[0]
    piece = block_rows // pieces
    shift = block_rows.bit_length() - 1

    def tab_copy(i):
        part = pl.ds(i * piece, piece)
        return pltpu.make_async_copy(table_ref.at[part], tab.at[part], tab_sem.at[i])

    for i in range(pieces):
        tab_copy(i).start()

    def ids_copy(c):
        return pltpu.make_async_remote_copy(
            src_ref=ids_ref,
            dst_ref=ids_all.at[mc],
            send_sem=ids_send.at[c],
            recv_sem=ids_recv.at[mc],
            device_id={"cols": c},
            device_id_type=MESH,
        )

    def ids_arrival(c):
        return pltpu.make_async_remote_copy(
            src_ref=ids_ref,
            dst_ref=ids_all.at[c],
            send_sem=ids_send.at[c],
            recv_sem=ids_recv.at[c],
            device_id={"cols": c},
            device_id_type=MESH,
        )

    def req_copy(r):
        return pltpu.make_async_remote_copy(
            src_ref=req.at[r],
            dst_ref=asked.at[mr],
            send_sem=req_send.at[r],
            recv_sem=req_recv.at[mr],
            device_id={"rows": r},
            device_id_type=MESH,
        )

    def req_arrival(r):
        return pltpu.make_async_remote_copy(
            src_ref=req.at[r],
            dst_ref=asked.at[r],
            send_sem=req_send.at[r],
            recv_sem=req_recv.at[r],
            device_id={"rows": r},
            device_id_type=MESH,
        )

    def row_copy(r):
        return pltpu.make_async_remote_copy(
            src_ref=outbox.at[r],
            dst_ref=ret_ref.at[mr],
            send_sem=row_send.at[r],
            recv_sem=row_recv.at[mr],
            device_id={"rows": r},
            device_id_type=MESH,
        )

    def row_arrival(r):
        return pltpu.make_async_remote_copy(
            src_ref=outbox.at[r],
            dst_ref=ret_ref.at[r],
            send_sem=row_send.at[r],
            recv_sem=row_recv.at[r],
            device_id={"rows": r},
            device_id_type=MESH,
        )

    barrier = pltpu.get_barrier_semaphore()
    for off in range(1, cols):
        pl.semaphore_signal(
            barrier, inc=1, device_id={"cols": lax.rem(mc + off, cols)}, device_id_type=MESH
        )
    for off in range(1, rows):
        pl.semaphore_signal(
            barrier, inc=1, device_id={"rows": lax.rem(mr + off, rows)}, device_id_type=MESH
        )
    pl.semaphore_wait(barrier, cols - 1 + rows - 1)

    for off in range(1, cols):
        ids_copy(lax.rem(mc + off, cols)).start()
    ids_all[mc] = ids_ref[...]

    step = 512
    for i in range(pieces):
        tab_copy(i).wait()

        def widen(k, carry):
            part = pl.ds(pl.multiple_of(i * piece + k * step, step), step)
            wide_tab[part, :] = tab[part, :].astype(F32)
            return carry

        lax.fori_loop(0, piece // step, widen, 0)

    for off in range(1, cols):
        ids_arrival(lax.rem(mc + off, cols)).wait_recv()
    for c in range(cols):
        for b in range(batch):
            for k in range(tiles):
                line = (c * batch + b) * tiles + k
                ids_s[line : line + 1, :] = ids_all[c, b : b + 1, k * LANES : (k + 1) * LANES]
    ids = ids_s[...]
    owner = lax.shift_right_logical(ids, shift)
    offset = ids - owner * block_rows

    src_lane = lax.broadcasted_iota(jnp.int32, (LANES, 2 * LANES), 0)
    dst_lane = lax.broadcasted_iota(jnp.int32, (LANES, 2 * LANES), 1)
    before = jnp.where(src_lane < dst_lane, 1.0, 0.0).astype(BF)
    line_a = lax.broadcasted_iota(jnp.int32, (lines, lines), 0)
    line_b = lax.broadcasted_iota(jnp.int32, (lines, lines), 1)
    above = jnp.where(line_b < line_a, 1.0, 0.0).astype(BF)
    rank = jnp.zeros((lines, LANES), F32)
    for r in range(rows):
        mine = owner == r
        counts = jnp.dot(
            jnp.where(mine, 1.0, 0.0).astype(BF), before, preferred_element_type=F32
        )
        earlier = jnp.dot(above, counts[:, LANES:].astype(BF), preferred_element_type=F32)
        rank = rank + jnp.where(mine, counts[:, :LANES] + earlier, 0.0)
    rank = rank.astype(jnp.int32)
    slot_ref[...] = owner * cap + rank
    group = owner * groups + lax.shift_right_logical(rank, 7)
    lane = rank - lax.shift_right_logical(rank, 7) * LANES
    high = lax.shift_right_logical(offset, 7)
    low = (offset - high * LANES).astype(F32)
    high = high.astype(F32)
    group_iota = lax.broadcasted_iota(jnp.int32, (rows * groups, LANES), 0)
    lane_iota = lax.broadcasted_iota(jnp.int32, (LANES, LANES), 0)
    for k in range(lines):
        part = slice(k * LANES, (k + 1) * LANES)
        line = slice(k, k + 1)
        left[:, part] = jnp.where(group[line] == group_iota, 1.0, 0.0).astype(BF)
        hit = lane[line] == lane_iota
        right[:LANES, part] = jnp.where(hit, high[line], 0.0).astype(BF)
        right[LANES:, part] = jnp.where(hit, low[line], 0.0).astype(BF)
    found = lax.dot_general(
        left[...], right[...], (((1,), (1,)), ((), ())), preferred_element_type=F32
    )
    found = (found[:, :LANES] * LANES + found[:, LANES:]).astype(jnp.int32)
    found = jnp.minimum(jnp.maximum(found, 0), block_rows - 1)
    req[...] = found.reshape(rows, groups, LANES)

    def over_rows(act):
        def body(i, carry):
            act(lax.rem(mr + i + 1, rows))
            return carry

        lax.fori_loop(0, rows - 1, body, 0)

    over_rows(lambda r: req_copy(r).start())
    asked[mr] = req[mr]
    over_rows(lambda r: req_arrival(r).wait_recv())
    to_smem = pltpu.make_async_copy(asked, asked_s, smem_sem)
    to_smem.start()
    to_smem.wait()

    own = pltpu.make_async_copy(outbox.at[mr], ret_ref.at[mr], own_sem)

    def serve(i, carry):
        dist = (i + 1) // 2
        off = rows // 2 + dist * (1 - 2 * lax.rem(i, 2))
        r = lax.rem(mr + off, rows)

        def some(g, count):
            for u in range(count):
                stage[u : u + 1, :] = wide_tab[pl.ds(asked_s[r, g, u], 1), :]
            part = pl.ds(pl.multiple_of(g * LANES, LANES), count)
            outbox[r, part, :] = stage[:count].astype(BF)

        def full_line(g, carry):
            some(g, LANES)
            return carry

        lax.fori_loop(0, cap // LANES, full_line, 0)
        if cap % LANES:
            some(cap // LANES, cap % LANES)

        @pl.when(i < rows - 1)
        def _():
            row_copy(r).start()

        return carry

    lax.fori_loop(0, rows, serve, 0)
    own.start()
    own.wait()
    over_rows(lambda r: row_arrival(r).wait_recv())
    for off in range(1, cols):
        ids_copy(lax.rem(mc + off, cols)).wait_send()
    over_rows(lambda r: req_copy(r).wait_send())
    over_rows(lambda r: row_copy(r).wait_send())


def fetch_call(rows, cols, cap, token_ids, table):
    batch, quarter = token_ids.shape
    tokens = batch * quarter * cols
    lines = tokens // LANES
    block_rows, width = table.shape
    assert block_rows & (block_rows - 1) == 0 and rows % 2 == 0
    groups = -(-cap // (8 * LANES)) * 8
    any_spec = pl.BlockSpec(memory_space=pl.ANY)
    vmem = pl.BlockSpec(memory_space=pltpu.VMEM)
    dma = pltpu.SemaphoreType.DMA
    return pl.pallas_call(
        functools.partial(fetch_kernel, rows, cols, cap),
        out_shape=(
            jax.ShapeDtypeStruct((rows, cap, width), BF),
            jax.ShapeDtypeStruct((lines, LANES), jnp.int32),
        ),
        in_specs=[vmem, any_spec],
        out_specs=(any_spec, vmem),
        scratch_shapes=[
            pltpu.VMEM((cols, batch, quarter), jnp.int32),
            pltpu.VMEM((lines, LANES), jnp.int32),
            pltpu.VMEM((rows * groups, tokens), BF),
            pltpu.VMEM((2 * LANES, tokens), BF),
            pltpu.VMEM((rows, groups, LANES), jnp.int32),
            pltpu.VMEM((rows, groups, LANES), jnp.int32),
            pltpu.SMEM((rows, groups, LANES), jnp.int32),
            pltpu.VMEM((block_rows, width), BF),
            pltpu.VMEM((block_rows, width), F32),
            pltpu.VMEM((LANES, width), F32),
            pltpu.VMEM((rows, cap, width), BF),
            dma((cols,)),
            dma((cols,)),
            dma((rows,)),
            dma((rows,)),
            dma((rows,)),
            dma((rows,)),
            dma((4,)),
            dma,
            dma,
        ],
        compiler_params=pltpu.CompilerParams(
            collective_id=1, has_side_effects=True, vmem_limit_bytes=60 * 1024 * 1024
        ),
    )(token_ids, table)


def local(token_ids, lengths, table, attn_gain, w_qkv, w_out, mlp_gain, w_in, w_down):
    batch_dev, quarter = token_ids.shape
    col_count = lax.axis_size("cols")
    row_count = lax.axis_size("rows")
    full_len = quarter * col_count
    token_count = batch_dev * full_len
    capacity = -(-(8 * token_count // (3 * row_count)) // 32) * 32
    returned, slots = fetch_call(row_count, col_count, capacity, token_ids, table)
    return layer_call(
        col_count, batch_dev, lengths, slots, returned,
        attn_gain, mlp_gain, w_qkv, w_out, w_in, w_down,
    )


def solution(mesh):
    in_specs = (P("rows", "cols"), P("rows"), P("rows", "cols"), P(), P(), P(), P(), P(), P())
    out_specs = P("rows", "cols", None)
    return jax.shard_map(local, mesh=mesh, in_specs=in_specs, out_specs=out_specs, check_vma=False)
```

```python
import functools

import jax
import jax.numpy as jnp
from jax import lax
from jax.experimental import pallas as pl
from jax.experimental.pallas import tpu as pltpu
from jax.sharding import PartitionSpec as P

HEADS = 8
LANES = 128
NEG = -1e30
SCORE_SCALE = 0.125 * 1.4426950408889634
MESH = pl.DeviceIdType.MESH
BF = jnp.bfloat16
F32 = jnp.float32


def rms_norm(values_f32, gain):
    mean_sq = jnp.mean(values_f32 * values_f32, axis=-1, keepdims=True)
    return values_f32 * lax.rsqrt(mean_sq + 1e-06) * gain


def whole_kernel(
    rows, cols, cap, ids_ref, lens_ref, table_ref, gain1, gain2, wqkv_h, wo_h, wi_h, wd_h, out_ref,
    ids_all, ids_s, slots_v, slots_s, left, right, req, asked, asked_s, tab, wide_tab, outbox, raw,
    stage, ebox, ebuf, hbuf, hstage, wqkv, wo, wi, wd, wq, wv, qm, k_s, v_s, m_s, l_s, acc,
    ids_send, ids_recv, req_send, req_recv, row_send, row_recv, tab_sem, smem_sem,
    send_sem, pass_sem, recv_sem, hsend_sem, hrecv_sem, w_sem,
):
    me = lax.axis_index("cols")
    mr = lax.axis_index("rows")
    batch, quarter = ids_ref.shape
    block_rows, width = table_ref.shape
    d = width * cols
    tiles = quarter // LANES
    lines = ids_s.shape[0]
    groups = req.shape[1]
    pieces = tab_sem.shape[0]
    piece = block_rows // pieces
    shift = block_rows.bit_length() - 1
    half = quarter // 2
    head_dim = LANES // 2
    group = cols // batch
    hist = me // group
    other = batch - 1 - hist
    inner = group - 1 + hist
    far_inner = group - 1 + other
    mate = hist * group + (group - 1 - lax.rem(me, group))
    is_inner = me == inner
    falling = hist == 0
    hi = jnp.where(is_inner, cols - 2, cols - 1)
    mate_hi = jnp.where(is_inner, cols - 1, cols - 2)
    q_sent = jnp.where(falling, hi, cols - 1 - hi)
    q_kept = cols - 1 - q_sent

    def tab_copy(i):
        part = pl.ds(i * piece, piece)
        return pltpu.make_async_copy(table_ref.at[part], tab.at[part], tab_sem.at[i])

    for i in range(pieces):
        tab_copy(i).start()
    loads = [
        pltpu.make_async_copy(src, dst, w_sem.at[i])
        for i, (src, dst) in enumerate(((wqkv_h, wqkv), (wo_h, wo), (wi_h, wi), (wd_h, wd)))
    ]

    def order(h, t):
        return jnp.where(h == 0, cols - 1 - t, t)

    def far_copy(j):
        return pltpu.make_async_remote_copy(
            src_ref=ebox.at[j],
            dst_ref=ebuf.at[me, j],
            send_sem=send_sem.at[0, j],
            recv_sem=recv_sem.at[me, j],
            device_id={"cols": far_inner},
            device_id_type=MESH,
        )

    def mate_copy(j):
        return pltpu.make_async_remote_copy(
            src_ref=ebuf.at[me, j],
            dst_ref=ebuf.at[me, j],
            send_sem=send_sem.at[1, j],
            recv_sem=recv_sem.at[me, j],
            device_id={"cols": mate},
            device_id_type=MESH,
        )

    def pass_copy(s, j):
        return pltpu.make_async_remote_copy(
            src_ref=ebuf.at[s, j],
            dst_ref=ebuf.at[s, j],
            send_sem=pass_sem.at[s, j],
            recv_sem=recv_sem.at[s, j],
            device_id={"cols": mate},
            device_id_type=MESH,
        )

    def hidden_copy():
        return pltpu.make_async_remote_copy(
            src_ref=hstage,
            dst_ref=hbuf.at[hist],
            send_sem=hsend_sem,
            recv_sem=hrecv_sem,
            device_id={"cols": q_sent},
            device_id_type=MESH,
        )

    def ids_copy(c):
        return pltpu.make_async_remote_copy(
            src_ref=ids_ref,
            dst_ref=ids_all.at[me],
            send_sem=ids_send.at[c],
            recv_sem=ids_recv.at[me],
            device_id={"cols": c},
            device_id_type=MESH,
        )

    def ids_arrival(c):
        return pltpu.make_async_remote_copy(
            src_ref=ids_ref,
            dst_ref=ids_all.at[c],
            send_sem=ids_send.at[c],
            recv_sem=ids_recv.at[c],
            device_id={"cols": c},
            device_id_type=MESH,
        )

    def req_copy(r):
        return pltpu.make_async_remote_copy(
            src_ref=req.at[r],
            dst_ref=asked.at[mr],
            send_sem=req_send.at[r],
            recv_sem=req_recv.at[mr],
            device_id={"rows": r},
            device_id_type=MESH,
        )

    def req_arrival(r):
        return pltpu.make_async_remote_copy(
            src_ref=req.at[r],
            dst_ref=asked.at[r],
            send_sem=req_send.at[r],
            recv_sem=req_recv.at[r],
            device_id={"rows": r},
            device_id_type=MESH,
        )

    def row_copy(r):
        return pltpu.make_async_remote_copy(
            src_ref=outbox.at[r],
            dst_ref=raw.at[mr],
            send_sem=row_send.at[r],
            recv_sem=row_recv.at[mr],
            device_id={"rows": r},
            device_id_type=MESH,
        )

    def row_arrival(r):
        return pltpu.make_async_remote_copy(
            src_ref=outbox.at[r],
            dst_ref=raw.at[r],
            send_sem=row_send.at[r],
            recv_sem=row_recv.at[r],
            device_id={"rows": r},
            device_id_type=MESH,
        )

    barrier = pltpu.get_barrier_semaphore()
    for off in range(1, cols):
        pl.semaphore_signal(
            barrier, inc=1, device_id={"cols": lax.rem(me + off, cols)}, device_id_type=MESH
        )
    for off in range(1, rows):
        pl.semaphore_signal(
            barrier, inc=1, device_id={"rows": lax.rem(mr + off, rows)}, device_id_type=MESH
        )
    pl.semaphore_wait(barrier, cols - 1 + rows - 1)

    for off in range(1, cols):
        ids_copy(lax.rem(me + off, cols)).start()
    for load in loads:
        load.start()
    ids_all[me] = ids_ref[...]

    step = 512
    for i in range(pieces):
        tab_copy(i).wait()

        def widen(k, carry):
            part = pl.ds(pl.multiple_of(i * piece + k * step, step), step)
            wide_tab[part, :] = tab[part, :].astype(F32)
            return carry

        lax.fori_loop(0, piece // step, widen, 0)

    for off in range(1, cols):
        ids_arrival(lax.rem(me + off, cols)).wait_recv()
    for c in range(cols):
        for b in range(batch):
            for k in range(tiles):
                line = (c * batch + b) * tiles + k
                ids_s[line : line + 1, :] = ids_all[c, b : b + 1, k * LANES : (k + 1) * LANES]
    ids = ids_s[...]
    owner = lax.shift_right_logical(ids, shift)
    offset = ids - owner * block_rows

    src_lane = lax.broadcasted_iota(jnp.int32, (LANES, 2 * LANES), 0)
    dst_lane = lax.broadcasted_iota(jnp.int32, (LANES, 2 * LANES), 1)
    before = jnp.where(src_lane < dst_lane, 1.0, 0.0).astype(BF)
    line_a = lax.broadcasted_iota(jnp.int32, (lines, lines), 0)
    line_b = lax.broadcasted_iota(jnp.int32, (lines, lines), 1)
    above = jnp.where(line_b < line_a, 1.0, 0.0).astype(BF)
    rank = jnp.zeros((lines, LANES), F32)
    for r in range(rows):
        mine = owner == r
        counts = jnp.dot(
            jnp.where(mine, 1.0, 0.0).astype(BF), before, preferred_element_type=F32
        )
        earlier = jnp.dot(above, counts[:, LANES:].astype(BF), preferred_element_type=F32)
        rank = rank + jnp.where(mine, counts[:, :LANES] + earlier, 0.0)
    rank = rank.astype(jnp.int32)
    slots_v[...] = jnp.minimum(jnp.maximum(owner * cap + rank, 0), rows * cap - 1)
    slot_group = owner * groups + lax.shift_right_logical(rank, 7)
    lane = rank - lax.shift_right_logical(rank, 7) * LANES
    high = lax.shift_right_logical(offset, 7)
    low = (offset - high * LANES).astype(F32)
    high = high.astype(F32)
    group_iota = lax.broadcasted_iota(jnp.int32, (rows * groups, LANES), 0)
    lane_iota = lax.broadcasted_iota(jnp.int32, (LANES, LANES), 0)
    for k in range(lines):
        part = slice(k * LANES, (k + 1) * LANES)
        line = slice(k, k + 1)
        left[:, part] = jnp.where(slot_group[line] == group_iota, 1.0, 0.0).astype(BF)
        hit = lane[line] == lane_iota
        right[:LANES, part] = jnp.where(hit, high[line], 0.0).astype(BF)
        right[LANES:, part] = jnp.where(hit, low[line], 0.0).astype(BF)
    found = lax.dot_general(
        left[...], right[...], (((1,), (1,)), ((), ())), preferred_element_type=F32
    )
    found = (found[:, :LANES] * LANES + found[:, LANES:]).astype(jnp.int32)
    found = jnp.minimum(jnp.maximum(found, 0), block_rows - 1)
    req[...] = found.reshape(rows, groups, LANES)

    def offset_of(i):
        return rows // 2 + (i + 1) // 2 * (1 - 2 * lax.rem(i, 2))

    def over_rows(act):
        def body(i, carry):
            act(lax.rem(mr + i + 1, rows))
            return carry

        lax.fori_loop(0, rows - 1, body, 0)

    over_rows(lambda r: req_copy(r).start())
    asked[mr] = req[mr]
    over_rows(lambda r: req_arrival(r).wait_recv())
    to_smem = pltpu.make_async_copy(asked, asked_s, smem_sem.at[0])
    slots_copy = pltpu.make_async_copy(slots_v, slots_s, smem_sem.at[1])
    to_smem.start()
    slots_copy.start()
    to_smem.wait()
    slots_copy.wait()

    def serve(i, carry):
        r = lax.rem(mr + offset_of(i), rows)

        def some(g, count):
            for u in range(count):
                stage[u : u + 1, :] = wide_tab[pl.ds(asked_s[r, g, u], 1), :]
            part = pl.ds(pl.multiple_of(g * LANES, LANES), count)
            outbox[r, part, :] = stage[:count].astype(BF)

        def full_line(g, carry):
            some(g, LANES)
            return carry

        lax.fori_loop(0, cap // LANES, full_line, 0)
        if cap % LANES:
            some(cap // LANES, cap % LANES)

        @pl.when(i < rows - 1)
        def _():
            row_copy(r).start()

        return carry

    lax.fori_loop(0, rows, serve, 0)

    loads[0].wait()
    wq[...] = wqkv[:, :d].astype(F32).T.astype(BF)
    wv[...] = wqkv[:, 2 * d :].astype(F32).T.astype(BF)
    for load in loads[1:]:
        load.wait()

    def widen_row(i, carry):
        r = lax.rem(mr + rows - offset_of(i), rows)
        part = pl.ds(pl.multiple_of(r * cap, 16), cap)

        @pl.when(i < rows - 1)
        def _():
            row_arrival(r).wait_recv()
            wide_tab[part, :] = raw[r].astype(F32)

        @pl.when(i == rows - 1)
        def _():
            wide_tab[part, :] = outbox[r].astype(F32)

        return carry

    lax.fori_loop(0, rows, widen_row, 0)


    def pick(t, carry):
        for side in range(2):
            h = other if side == 0 else hist
            j = order(h, t)
            line = (j * batch + h) * tiles
            for k in range(tiles):
                for u in range(LANES):
                    stage[u : u + 1, :] = wide_tab[pl.ds(slots_s[line + k, u], 1), :]
                part = slice(k * LANES, (k + 1) * LANES)
                if side == 0:
                    ebox[j, part, :] = stage[...].astype(BF)
                else:
                    ebuf[me, j, part, :] = stage[...].astype(BF)
            if side == 0:
                far_copy(j).start()
            else:

                @pl.when(j <= mate_hi)
                def _():
                    mate_copy(j).start()

        return carry

    lax.fori_loop(0, cols, pick, 0)
    dims_nt = (((1,), (1,)), ((), ()))
    length = lens_ref[hist]

    def embedded(j):
        parts = [ebuf[s, j] for s in range(cols)]
        return jnp.concatenate(parts, axis=1).astype(F32)

    def flash(slot, h, k_blk, v_t, q0, qn, causal):
        s = jnp.dot(k_blk, qm[slot, h, :, q0 : q0 + qn], preferred_element_type=F32)
        kn = k_blk.shape[0]
        if causal:
            key_pos = lax.broadcasted_iota(jnp.int32, (kn, qn), 0)
            query_pos = lax.broadcasted_iota(jnp.int32, (kn, qn), 1) + q0
            s = jnp.where(key_pos <= query_pos, s, NEG)
        m_old = m_s[slot, h, :, q0 : q0 + qn]
        m_new = jnp.maximum(m_old, jnp.max(s, axis=0, keepdims=True))
        probs = jnp.exp2(s - m_new)
        alpha = jnp.exp2(m_old - m_new)
        m_s[slot, h, :, q0 : q0 + qn] = m_new
        l_s[slot, h, :, q0 : q0 + qn] = l_s[slot, h, :, q0 : q0 + qn] * alpha + jnp.sum(
            probs, axis=0, keepdims=True
        )
        acc[slot, h, :, q0 : q0 + qn] = acc[slot, h, :, q0 : q0 + qn] * alpha + jnp.dot(
            v_t, probs.astype(BF), preferred_element_type=F32
        )

    def attend(slot, j, causal):
        def pair(p, carry):
            for side in range(2):
                h = 2 * p + side
                wide_p = pl.ds(pl.multiple_of(p * 2 * LANES, 2 * LANES), 2 * LANES)
                part = pl.ds(pl.multiple_of(h * head_dim, head_dim), head_dim)
                if causal:
                    flash(slot, h, k_s[j, :half, wide_p], v_s[j, part, :half], 0, half, True)
                    flash(slot, h, k_s[j, :, wide_p], v_s[j, part, :], half, half, True)
                else:
                    flash(slot, h, k_s[j, :, wide_p], v_s[j, part, :], 0, quarter, False)
            return carry

        lax.fori_loop(0, HEADS // 2, pair, 0)

    def arrive(j):
        for s in range(cols):
            far = s // group == other

            @pl.when(far | ((s != me) & (j <= hi)))
            def _():
                pass_copy(s, j).wait_recv()

            @pl.when(is_inner & far)
            def _():
                pass_copy(s, j).start()

    def project(j):
        normed = rms_norm(embedded(j), gain1[...]).astype(BF)
        keys = jnp.dot(normed, wqkv[:, d : 2 * d], preferred_element_type=F32).astype(BF)
        row = lax.broadcasted_iota(jnp.int32, (quarter, LANES), 0)
        lane = lax.broadcasted_iota(jnp.int32, (quarter, LANES), 1)
        dead = (lane == 0) & (row >= length - j * quarter)
        bias = jnp.where(dead, NEG, 0.0).astype(BF)
        for p in range(HEADS // 2):
            k_s[j, :, 2 * p * LANES : (2 * p + 1) * LANES] = keys[:, p * LANES : (p + 1) * LANES]
            k_s[j, :, (2 * p + 1) * LANES : (2 * p + 2) * LANES] = bias
        v_s[j] = lax.dot_general(wv[...], normed, dims_nt, preferred_element_type=F32).astype(BF)

        @pl.when((j == q_sent) | (j == q_kept))
        def _():
            slot = jnp.where(j == q_sent, 0, 1)
            q_t = lax.dot_general(wq[...], normed, dims_nt, preferred_element_type=F32)
            q_t = (q_t * SCORE_SCALE).astype(BF)
            zero = jnp.zeros((head_dim, quarter), BF)
            one_row = lax.broadcasted_iota(jnp.int32, (LANES, quarter), 0) == 0
            one_row = jnp.where(one_row, 1.0, 0.0).astype(BF)
            for h in range(HEADS):
                mine = q_t[h * head_dim : (h + 1) * head_dim]
                pair = (mine, zero) if h % 2 == 0 else (zero, mine)
                qm[slot, h] = jnp.concatenate(pair + (one_row,), axis=0)
            m_s[slot] = jnp.full(m_s.shape[1:], NEG, F32)
            l_s[slot] = jnp.zeros(l_s.shape[1:], F32)
            acc[slot] = jnp.zeros(acc.shape[1:], F32)

    def step(t, carry):
        last = t == cols
        j = order(hist, jnp.minimum(t, cols - 1))

        @pl.when(t < cols)
        def _():
            arrive(j)

            @pl.when((t == cols - 1) & (hist > 0) & (me != inner))
            def _():
                hidden_copy().start()

            @pl.when(j <= hi)
            def _():
                project(j)

        slot = jnp.where(last, 1, 0)
        q = jnp.where(last, q_kept, q_sent)
        whole = last | ((hist > 0) & (j == q_sent))
        piece = (hist == 0) & (j <= q_sent) & (t < cols)
        count = jnp.where(whole, q + 1, jnp.where(piece, 1, 0))
        first = jnp.where(whole, q, j)

        def unit(i, carry):
            key = first - i

            @pl.when(key == q)
            def _():
                attend(slot, key, True)

            @pl.when(key < q)
            def _():
                attend(slot, key, False)

            @pl.when(key == 0)
            def _():
                att_t = (acc[slot] / l_s[slot]).reshape(HEADS * head_dim, quarter)
                attended = att_t.T.astype(BF)
                hidden = embedded(q) + jnp.dot(attended, wo[...], preferred_element_type=F32)
                hidden = hidden.astype(BF)

                @pl.when(last)
                def _():
                    hbuf[hist] = hidden

                @pl.when(t < cols)
                def _():
                    hstage[...] = hidden

                    @pl.when(falling | is_inner)
                    def _():
                        hidden_copy().start()

            return carry

        lax.fori_loop(0, count, unit, 0)
        return carry

    lax.fori_loop(0, cols + 1, step, 0)

    def mlp(i, carry):
        h = jnp.where(i == 0, hist, other)

        @pl.when(i > 0)
        def _():
            hidden_copy().wait_recv()

        hidden = hbuf[h].astype(F32)
        normed_two = rms_norm(hidden, gain2[...]).astype(BF)
        ff = wd.shape[0]
        tile = 512
        total = hidden
        for f in range(0, ff, tile):
            gate = jnp.dot(normed_two, wi[:, f : f + tile], preferred_element_type=F32)
            up = jnp.dot(normed_two, wi[:, ff + f : ff + f + tile], preferred_element_type=F32)
            act = (gate / (1.0 + jnp.exp(-gate)) * up).astype(BF)
            total = total + jnp.dot(act, wd[f : f + tile, :], preferred_element_type=F32)
        out_ref[h] = total.astype(BF)
        return carry

    lax.fori_loop(0, batch, mlp, 0)
    for j in range(cols):
        far_copy(j).wait_send()

        @pl.when(j <= mate_hi)
        def _():
            mate_copy(j).wait_send()

        for s in range(cols):

            @pl.when(is_inner & (s // group == other))
            def _():
                pass_copy(s, j).wait_send()

    hidden_copy().wait_send()
    for off in range(1, cols):
        ids_copy(lax.rem(me + off, cols)).wait_send()
    over_rows(lambda r: req_copy(r).wait_send())
    over_rows(lambda r: row_copy(r).wait_send())


def whole_call(rows, cols, cap, token_ids, lengths, table, gain1, gain2, w_qkv, w_out, w_in, w_down):
    batch, quarter = token_ids.shape
    tokens = batch * quarter * cols
    lines = tokens // LANES
    block_rows, width = table.shape
    d = width * cols
    head_dim = d // HEADS
    assert batch == 2 and cols == 2 * batch and rows % 2 == 0
    assert block_rows & (block_rows - 1) == 0 and rows * cap <= block_rows
    groups = -(-cap // (8 * LANES)) * 8
    any_spec = pl.BlockSpec(memory_space=pl.ANY)
    vmem = pl.BlockSpec(memory_space=pltpu.VMEM)
    smem = pl.BlockSpec(memory_space=pltpu.SMEM)
    dma = pltpu.SemaphoreType.DMA
    i32 = jnp.int32
    return pl.pallas_call(
        functools.partial(whole_kernel, rows, cols, cap),
        out_shape=jax.ShapeDtypeStruct((batch, quarter, d), BF),
        in_specs=[vmem, smem, any_spec, vmem, vmem] + [any_spec] * 4,
        out_specs=vmem,
        scratch_shapes=[
            pltpu.VMEM((cols, batch, quarter), i32),
            pltpu.VMEM((lines, LANES), i32),
            pltpu.VMEM((lines, LANES), i32),
            pltpu.SMEM((lines, LANES), i32),
            pltpu.VMEM((rows * groups, tokens), BF),
            pltpu.VMEM((2 * LANES, tokens), BF),
            pltpu.VMEM((rows, groups, LANES), i32),
            pltpu.VMEM((rows, groups, LANES), i32),
            pltpu.SMEM((rows, groups, LANES), i32),
            pltpu.VMEM((block_rows, width), BF),
            pltpu.VMEM((block_rows, width), F32),
            pltpu.VMEM((rows, cap, width), BF),
            pltpu.VMEM((rows, cap, width), BF),
            pltpu.VMEM((LANES, width), F32),
            pltpu.VMEM((cols, quarter, width), BF),
            pltpu.VMEM((cols, cols, quarter, width), BF),
            pltpu.VMEM((batch, quarter, d), BF),
            pltpu.VMEM((quarter, d), BF),
            pltpu.VMEM(w_qkv.shape, BF),
            pltpu.VMEM(w_out.shape, BF),
            pltpu.VMEM(w_in.shape, BF),
            pltpu.VMEM(w_down.shape, BF),
            pltpu.VMEM((d, d), BF),
            pltpu.VMEM((d, d), BF),
            pltpu.VMEM((2, HEADS, 4 * head_dim, quarter), BF),
            pltpu.VMEM((cols, quarter, 2 * d), BF),
            pltpu.VMEM((cols, d, quarter), BF),
            pltpu.VMEM((2, HEADS, 1, quarter), F32),
            pltpu.VMEM((2, HEADS, 1, quarter), F32),
            pltpu.VMEM((2, HEADS, head_dim, quarter), F32),
            dma((cols,)),
            dma((cols,)),
            dma((rows,)),
            dma((rows,)),
            dma((rows,)),
            dma((rows,)),
            dma((4,)),
            dma((2,)),
            dma((2, cols)),
            dma((cols, cols)),
            dma((cols, cols)),
            dma,
            dma,
            dma((4,)),
        ],
        compiler_params=pltpu.CompilerParams(
            collective_id=0, has_side_effects=True, vmem_limit_bytes=63 * 1024 * 1024
        ),
    )(token_ids, lengths, table, gain1.reshape(1, d), gain2.reshape(1, d), w_qkv, w_out, w_in, w_down)


def local(token_ids, lengths, table, attn_gain, w_qkv, w_out, mlp_gain, w_in, w_down):
    batch_dev, quarter = token_ids.shape
    col_count = lax.axis_size("cols")
    row_count = lax.axis_size("rows")
    token_count = batch_dev * quarter * col_count
    capacity = -(-(8 * token_count // (3 * row_count)) // 32) * 32
    return whole_call(
        row_count, col_count, capacity, token_ids, lengths, table,
        attn_gain, mlp_gain, w_qkv, w_out, w_in, w_down,
    )


def solution(mesh):
    in_specs = (P("rows", "cols"), P("rows"), P("rows", "cols"), P(), P(), P(), P(), P(), P())
    out_specs = P("rows", "cols", None)
    return jax.shard_map(local, mesh=mesh, in_specs=in_specs, out_specs=out_specs, check_vma=False)
```

```python
import functools

import jax
import jax.numpy as jnp
from jax import lax
from jax.experimental import pallas as pl
from jax.experimental.pallas import tpu as pltpu
from jax.sharding import PartitionSpec as P

HEADS = 8
LANES = 128
NEG = -1e30
SCORE_SCALE = 0.125 * 1.4426950408889634
MESH = pl.DeviceIdType.MESH
BF = jnp.bfloat16
F32 = jnp.float32


def rms_norm(values_f32, gain):
    mean_sq = jnp.mean(values_f32 * values_f32, axis=-1, keepdims=True)
    return values_f32 * lax.rsqrt(mean_sq + 1e-06) * gain


def whole_kernel(
    rows, cols, cap, ids_ref, lens_ref, table_ref, gain1, gain2, wqkv_h, wo_h, wi_h, wd_h, out_ref,
    ids_all, ids_s, slots_v, slots_s, left, right, req, asked, asked_s, tab, wide_tab, outbox, raw,
    stage, ebox, ebuf, hbuf, hstage, wqkv, wo, wi, wd, wq, wv, qm, k_s, v_s, m_s, l_s, acc, s_buf,
    ids_send, ids_recv, req_send, req_recv, row_send, row_recv, tab_sem, smem_sem,
    send_sem, pass_sem, recv_sem, hsend_sem, hrecv_sem, w_sem,
):
    me = lax.axis_index("cols")
    mr = lax.axis_index("rows")
    batch, quarter = ids_ref.shape
    block_rows, width = table_ref.shape
    d = width * cols
    tiles = quarter // LANES
    lines = ids_s.shape[0]
    groups = req.shape[1]
    pieces = tab_sem.shape[0]
    piece = block_rows // pieces
    shift = block_rows.bit_length() - 1
    half = quarter // 2
    head_dim = LANES // 2
    group = cols // batch
    hist = me // group
    other = batch - 1 - hist
    inner = group - 1 + hist
    far_inner = group - 1 + other
    mate = hist * group + (group - 1 - lax.rem(me, group))
    is_inner = me == inner
    falling = hist == 0
    low = cols // 2 - 1
    hi = jnp.where(is_inner, cols - 1, low)
    mate_hi = jnp.where(is_inner, low, cols - 1)

    def query_of(slot):
        return jnp.where(is_inner, hi - slot, jnp.where(falling, hi - slot, slot))

    def tab_copy(i):
        part = pl.ds(i * piece, piece)
        return pltpu.make_async_copy(table_ref.at[part], tab.at[part], tab_sem.at[i])

    for i in range(pieces):
        tab_copy(i).start()
    loads = [
        pltpu.make_async_copy(src, dst, w_sem.at[i])
        for i, (src, dst) in enumerate(((wqkv_h, wqkv), (wo_h, wo), (wi_h, wi), (wd_h, wd)))
    ]

    def order(h, t):
        falls = jnp.where(t <= low + 1, low + 1 - t, t - 1)
        return jnp.where(t == 0, cols - 1, jnp.where(h == 0, falls, t - 1))

    def far_copy(j):
        return pltpu.make_async_remote_copy(
            src_ref=ebox.at[j],
            dst_ref=ebuf.at[me, j],
            send_sem=send_sem.at[0, j],
            recv_sem=recv_sem.at[me, j],
            device_id={"cols": far_inner},
            device_id_type=MESH,
        )

    def mate_copy(j):
        return pltpu.make_async_remote_copy(
            src_ref=ebuf.at[me, j],
            dst_ref=ebuf.at[me, j],
            send_sem=send_sem.at[1, j],
            recv_sem=recv_sem.at[me, j],
            device_id={"cols": mate},
            device_id_type=MESH,
        )

    def pass_copy(s, j):
        return pltpu.make_async_remote_copy(
            src_ref=ebuf.at[s, j],
            dst_ref=ebuf.at[s, j],
            send_sem=pass_sem.at[s, j],
            recv_sem=recv_sem.at[s, j],
            device_id={"cols": mate},
            device_id_type=MESH,
        )

    def hidden_copy(slot):
        return pltpu.make_async_remote_copy(
            src_ref=hstage.at[slot],
            dst_ref=hbuf.at[hist],
            send_sem=hsend_sem.at[slot],
            recv_sem=hrecv_sem.at[hist],
            device_id={"cols": query_of(slot)},
            device_id_type=MESH,
        )

    def hidden_arrival(h):
        return pltpu.make_async_remote_copy(
            src_ref=hstage.at[0],
            dst_ref=hbuf.at[h],
            send_sem=hsend_sem.at[0],
            recv_sem=hrecv_sem.at[h],
            device_id={"cols": mate},
            device_id_type=MESH,
        )

    def ids_copy(c):
        return pltpu.make_async_remote_copy(
            src_ref=ids_ref,
            dst_ref=ids_all.at[me],
            send_sem=ids_send.at[c],
            recv_sem=ids_recv.at[me],
            device_id={"cols": c},
            device_id_type=MESH,
        )

    def ids_arrival(c):
        return pltpu.make_async_remote_copy(
            src_ref=ids_ref,
            dst_ref=ids_all.at[c],
            send_sem=ids_send.at[c],
            recv_sem=ids_recv.at[c],
            device_id={"cols": c},
            device_id_type=MESH,
        )

    def req_copy(r):
        return pltpu.make_async_remote_copy(
            src_ref=req.at[r],
            dst_ref=asked.at[mr],
            send_sem=req_send.at[r],
            recv_sem=req_recv.at[mr],
            device_id={"rows": r},
            device_id_type=MESH,
        )

    def req_arrival(r):
        return pltpu.make_async_remote_copy(
            src_ref=req.at[r],
            dst_ref=asked.at[r],
            send_sem=req_send.at[r],
            recv_sem=req_recv.at[r],
            device_id={"rows": r},
            device_id_type=MESH,
        )

    def row_copy(r):
        return pltpu.make_async_remote_copy(
            src_ref=outbox.at[r],
            dst_ref=raw.at[mr],
            send_sem=row_send.at[r],
            recv_sem=row_recv.at[mr],
            device_id={"rows": r},
            device_id_type=MESH,
        )

    def row_arrival(r):
        return pltpu.make_async_remote_copy(
            src_ref=outbox.at[r],
            dst_ref=raw.at[r],
            send_sem=row_send.at[r],
            recv_sem=row_recv.at[r],
            device_id={"rows": r},
            device_id_type=MESH,
        )

    barrier = pltpu.get_barrier_semaphore()
    for off in range(1, cols):
        pl.semaphore_signal(
            barrier, inc=1, device_id={"cols": lax.rem(me + off, cols)}, device_id_type=MESH
        )
    for off in range(1, rows):
        pl.semaphore_signal(
            barrier, inc=1, device_id={"rows": lax.rem(mr + off, rows)}, device_id_type=MESH
        )
    pl.semaphore_wait(barrier, cols - 1 + rows - 1)

    for off in range(1, cols):
        ids_copy(lax.rem(me + off, cols)).start()
    for load in loads:
        load.start()
    ids_all[me] = ids_ref[...]

    step = 512
    for i in range(pieces):
        tab_copy(i).wait()

        def widen(k, carry):
            part = pl.ds(pl.multiple_of(i * piece + k * step, step), step)
            wide_tab[part, :] = tab[part, :].astype(F32)
            return carry

        lax.fori_loop(0, piece // step, widen, 0)

    for off in range(1, cols):
        ids_arrival(lax.rem(me + off, cols)).wait_recv()
    for c in range(cols):
        for b in range(batch):
            for k in range(tiles):
                line = (c * batch + b) * tiles + k
                ids_s[line : line + 1, :] = ids_all[c, b : b + 1, k * LANES : (k + 1) * LANES]
    ids = ids_s[...]
    owner = lax.shift_right_logical(ids, shift)
    offset = ids - owner * block_rows

    src_lane = lax.broadcasted_iota(jnp.int32, (LANES, 2 * LANES), 0)
    dst_lane = lax.broadcasted_iota(jnp.int32, (LANES, 2 * LANES), 1)
    before = jnp.where(src_lane < dst_lane, 1.0, 0.0).astype(BF)
    line_a = lax.broadcasted_iota(jnp.int32, (lines, lines), 0)
    line_b = lax.broadcasted_iota(jnp.int32, (lines, lines), 1)
    above = jnp.where(line_b < line_a, 1.0, 0.0).astype(BF)
    rank = jnp.zeros((lines, LANES), F32)
    for r in range(rows):
        mine = owner == r
        counts = jnp.dot(
            jnp.where(mine, 1.0, 0.0).astype(BF), before, preferred_element_type=F32
        )
        earlier = jnp.dot(above, counts[:, LANES:].astype(BF), preferred_element_type=F32)
        rank = rank + jnp.where(mine, counts[:, :LANES] + earlier, 0.0)
    rank = rank.astype(jnp.int32)
    slots_v[...] = jnp.minimum(jnp.maximum(owner * cap + rank, 0), rows * cap - 1)
    slot_group = owner * groups + lax.shift_right_logical(rank, 7)
    lane = rank - lax.shift_right_logical(rank, 7) * LANES
    high = lax.shift_right_logical(offset, 7)
    low_part = (offset - high * LANES).astype(F32)
    high = high.astype(F32)
    group_iota = lax.broadcasted_iota(jnp.int32, (rows * groups, LANES), 0)
    lane_iota = lax.broadcasted_iota(jnp.int32, (LANES, LANES), 0)
    for k in range(lines):
        part = slice(k * LANES, (k + 1) * LANES)
        line = slice(k, k + 1)
        left[:, part] = jnp.where(slot_group[line] == group_iota, 1.0, 0.0).astype(BF)
        hit = lane[line] == lane_iota
        right[:LANES, part] = jnp.where(hit, high[line], 0.0).astype(BF)
        right[LANES:, part] = jnp.where(hit, low_part[line], 0.0).astype(BF)
    found = lax.dot_general(
        left[...], right[...], (((1,), (1,)), ((), ())), preferred_element_type=F32
    )
    found = (found[:, :LANES] * LANES + found[:, LANES:]).astype(jnp.int32)
    found = jnp.minimum(jnp.maximum(found, 0), block_rows - 1)
    req[...] = found.reshape(rows, groups, LANES)

    def offset_of(i):
        return rows // 2 + (i + 1) // 2 * (1 - 2 * lax.rem(i, 2))

    def over_rows(act):
        def body(i, carry):
            act(lax.rem(mr + i + 1, rows))
            return carry

        lax.fori_loop(0, rows - 1, body, 0)

    over_rows(lambda r: req_copy(r).start())
    asked[mr] = req[mr]
    over_rows(lambda r: req_arrival(r).wait_recv())
    to_smem = pltpu.make_async_copy(asked, asked_s, smem_sem.at[0])
    slots_copy = pltpu.make_async_copy(slots_v, slots_s, smem_sem.at[1])
    to_smem.start()
    slots_copy.start()
    to_smem.wait()
    slots_copy.wait()

    def serve(i, carry):
        r = lax.rem(mr + offset_of(i), rows)

        def some(g, count):
            for u in range(count):
                stage[u : u + 1, :] = wide_tab[pl.ds(asked_s[r, g, u], 1), :]
            part = pl.ds(pl.multiple_of(g * LANES, LANES), count)
            outbox[r, part, :] = stage[:count].astype(BF)

        def full_line(g, carry):
            some(g, LANES)
            return carry

        lax.fori_loop(0, cap // LANES, full_line, 0)
        if cap % LANES:
            some(cap // LANES, cap % LANES)

        @pl.when(i < rows - 1)
        def _():
            row_copy(r).start()

        return carry

    lax.fori_loop(0, rows, serve, 0)

    loads[0].wait()
    wq[...] = wqkv[:, :d].astype(F32).T.astype(BF)
    wv[...] = wqkv[:, 2 * d :].astype(F32).T.astype(BF)
    for load in loads[1:]:
        load.wait()

    def widen_row(i, carry):
        r = lax.rem(mr + rows - offset_of(i), rows)
        part = pl.ds(pl.multiple_of(r * cap, 16), cap)

        @pl.when(i < rows - 1)
        def _():
            row_arrival(r).wait_recv()
            wide_tab[part, :] = raw[r].astype(F32)

        @pl.when(i == rows - 1)
        def _():
            wide_tab[part, :] = outbox[r].astype(F32)

        return carry

    lax.fori_loop(0, rows, widen_row, 0)


    def pick(t, carry):
        for side in range(2):
            h = other if side == 0 else hist
            j = order(h, t)
            line = (j * batch + h) * tiles
            for k in range(tiles):
                for u in range(LANES):
                    stage[u : u + 1, :] = wide_tab[pl.ds(slots_s[line + k, u], 1), :]
                part = slice(k * LANES, (k + 1) * LANES)
                if side == 0:
                    ebox[j, part, :] = stage[...].astype(BF)
                else:
                    ebuf[me, j, part, :] = stage[...].astype(BF)
            if side == 0:
                far_copy(j).start()
            else:

                @pl.when(j <= mate_hi)
                def _():
                    mate_copy(j).start()

        return carry

    lax.fori_loop(0, cols, pick, 0)
    dims_nt = (((1,), (1,)), ((), ()))
    length = lens_ref[hist]

    def embedded(j):
        parts = [ebuf[s, j] for s in range(cols)]
        return jnp.concatenate(parts, axis=1).astype(F32)

    def attend(slot, j, causal):
        if causal:
            items = [(h, n, n - half, half) for h in range(HEADS) for n in (half, quarter)]
        else:
            items = [(h, quarter, 0, quarter) for h in range(HEADS)]

        def scores(at):
            h, kn, q0, qn = items[at]
            k_blk = k_s[j, :kn, (h // 2) * 2 * LANES : (h // 2 + 1) * 2 * LANES]
            s = jnp.dot(k_blk, qm[slot, h, :, q0 : q0 + qn], preferred_element_type=F32)
            if causal:
                key_pos = lax.broadcasted_iota(jnp.int32, (kn, qn), 0)
                query_pos = lax.broadcasted_iota(jnp.int32, (kn, qn), 1) + q0
                s = jnp.where(key_pos <= query_pos, s, NEG)
            s_buf[at % 2, :kn, :qn] = s
            return jnp.max(s, axis=0, keepdims=True)

        top = scores(0)
        for at, (h, kn, q0, qn) in enumerate(items):
            next_top = scores(at + 1) if at + 1 < len(items) else None
            cut = slice(q0, q0 + qn)
            m_old = m_s[slot, h, :, cut]
            m_new = jnp.maximum(m_old, top)
            probs = jnp.exp2(s_buf[at % 2, :kn, :qn] - m_new)
            alpha = jnp.exp2(m_old - m_new)
            m_s[slot, h, :, cut] = m_new
            l_s[slot, h, :, cut] = l_s[slot, h, :, cut] * alpha + jnp.sum(
                probs, axis=0, keepdims=True
            )
            v_t = v_s[j, h * head_dim : (h + 1) * head_dim, :kn]
            acc[slot, h, :, cut] = acc[slot, h, :, cut] * alpha + jnp.dot(
                v_t, probs.astype(BF), preferred_element_type=F32
            )
            top = next_top

    def arrive(j):
        for s in range(cols):
            far = s // group == other

            @pl.when((s != me) & (j <= hi))
            def _():
                pass_copy(s, j).wait_recv()

            @pl.when(is_inner & far & (j <= low))
            def _():
                pass_copy(s, j).start()

    def project(j):
        normed = rms_norm(embedded(j), gain1[...]).astype(BF)
        keys = jnp.dot(normed, wqkv[:, d : 2 * d], preferred_element_type=F32).astype(BF)
        row = lax.broadcasted_iota(jnp.int32, (quarter, LANES), 0)
        lane = lax.broadcasted_iota(jnp.int32, (quarter, LANES), 1)
        dead = (lane == 0) & (row >= length - j * quarter)
        bias = jnp.where(dead, NEG, 0.0).astype(BF)
        for p in range(HEADS // 2):
            k_s[j, :, 2 * p * LANES : (2 * p + 1) * LANES] = keys[:, p * LANES : (p + 1) * LANES]
            k_s[j, :, (2 * p + 1) * LANES : (2 * p + 2) * LANES] = bias
        v_s[j] = lax.dot_general(wv[...], normed, dims_nt, preferred_element_type=F32).astype(BF)

        @pl.when((j == query_of(0)) | (j == query_of(1)))
        def _():
            slot = jnp.where(j == query_of(0), 0, 1)
            q_t = lax.dot_general(wq[...], normed, dims_nt, preferred_element_type=F32)
            q_t = (q_t * SCORE_SCALE).astype(BF)
            zero = jnp.zeros((head_dim, quarter), BF)
            one_row = lax.broadcasted_iota(jnp.int32, (LANES, quarter), 0) == 0
            one_row = jnp.where(one_row, 1.0, 0.0).astype(BF)
            for h in range(HEADS):
                mine = q_t[h * head_dim : (h + 1) * head_dim]
                pair = (mine, zero) if h % 2 == 0 else (zero, mine)
                qm[slot, h] = jnp.concatenate(pair + (one_row,), axis=0)
            m_s[slot] = jnp.full(m_s.shape[1:], NEG, F32)
            l_s[slot] = jnp.zeros(l_s.shape[1:], F32)
            acc[slot] = jnp.zeros(acc.shape[1:], F32)

    def step(t, carry):
        j = order(hist, t)

        @pl.when(j <= hi)
        def _():
            arrive(j)
            project(j)

        def query_step(slot, carry):
            q = query_of(slot)
            known = (q == cols - 1) | (falling & (q == low))
            fresh = jnp.where(known, 1, q + 1)
            count = jnp.where(j == q, fresh, jnp.where(known & (j < q), 1, 0))
            last_key = jnp.where(falling & (q == low), 0, q)
            done = jnp.where(q == cols - 1, t == cols - 1, j == last_key)

            def unit(i, carry):
                key = j - i

                @pl.when(key == q)
                def _():
                    attend(slot, key, True)

                @pl.when(key < q)
                def _():
                    attend(slot, key, False)

                return carry

            lax.fori_loop(0, count, unit, 0)

            @pl.when(done)
            def _():
                att_t = (acc[slot] / l_s[slot]).reshape(HEADS * head_dim, quarter)
                attended = att_t.T.astype(BF)
                hidden = embedded(q) + jnp.dot(attended, wo[...], preferred_element_type=F32)
                hidden = hidden.astype(BF)

                @pl.when(q == me)
                def _():
                    hbuf[hist] = hidden

                @pl.when(q != me)
                def _():
                    hstage[slot] = hidden
                    hidden_copy(slot).start()

            return carry

        @pl.when(j <= hi)
        def _():
            lax.fori_loop(0, 2, query_step, 0)

        return carry

    lax.fori_loop(0, cols, step, 0)

    def mlp(i, carry):
        first = jnp.where(falling | is_inner, hist, other)
        h = jnp.where(i == 0, first, batch - 1 - first)

        @pl.when((h != hist) | ((query_of(0) != me) & (query_of(1) != me)))
        def _():
            hidden_arrival(h).wait_recv()

        hidden = hbuf[h].astype(F32)
        normed_two = rms_norm(hidden, gain2[...]).astype(BF)
        ff = wd.shape[0]
        tile = 512
        total = hidden
        for f in range(0, ff, tile):
            gate = jnp.dot(normed_two, wi[:, f : f + tile], preferred_element_type=F32)
            up = jnp.dot(normed_two, wi[:, ff + f : ff + f + tile], preferred_element_type=F32)
            act = (gate / (1.0 + jnp.exp(-gate)) * up).astype(BF)
            total = total + jnp.dot(act, wd[f : f + tile, :], preferred_element_type=F32)
        out_ref[h] = total.astype(BF)
        return carry

    lax.fori_loop(0, batch, mlp, 0)
    for j in range(cols):
        far_copy(j).wait_send()

        @pl.when(j <= mate_hi)
        def _():
            mate_copy(j).wait_send()

        for s in range(cols):

            @pl.when(is_inner & (s // group == other) & (j <= low))
            def _():
                pass_copy(s, j).wait_send()

    for slot in range(2):

        @pl.when(query_of(slot) != me)
        def _():
            hidden_copy(slot).wait_send()

    for off in range(1, cols):
        ids_copy(lax.rem(me + off, cols)).wait_send()
    over_rows(lambda r: req_copy(r).wait_send())
    over_rows(lambda r: row_copy(r).wait_send())


def whole_call(rows, cols, cap, token_ids, lengths, table, gain1, gain2, w_qkv, w_out, w_in, w_down):
    batch, quarter = token_ids.shape
    tokens = batch * quarter * cols
    lines = tokens // LANES
    block_rows, width = table.shape
    d = width * cols
    head_dim = d // HEADS
    assert batch == 2 and cols == 2 * batch and rows % 2 == 0
    assert block_rows & (block_rows - 1) == 0 and rows * cap <= block_rows
    groups = -(-cap // (8 * LANES)) * 8
    any_spec = pl.BlockSpec(memory_space=pl.ANY)
    vmem = pl.BlockSpec(memory_space=pltpu.VMEM)
    smem = pl.BlockSpec(memory_space=pltpu.SMEM)
    dma = pltpu.SemaphoreType.DMA
    i32 = jnp.int32
    return pl.pallas_call(
        functools.partial(whole_kernel, rows, cols, cap),
        out_shape=jax.ShapeDtypeStruct((batch, quarter, d), BF),
        in_specs=[vmem, smem, any_spec, vmem, vmem] + [any_spec] * 4,
        out_specs=vmem,
        scratch_shapes=[
            pltpu.VMEM((cols, batch, quarter), i32),
            pltpu.VMEM((lines, LANES), i32),
            pltpu.VMEM((lines, LANES), i32),
            pltpu.SMEM((lines, LANES), i32),
            pltpu.VMEM((rows * groups, tokens), BF),
            pltpu.VMEM((2 * LANES, tokens), BF),
            pltpu.VMEM((rows, groups, LANES), i32),
            pltpu.VMEM((rows, groups, LANES), i32),
            pltpu.SMEM((rows, groups, LANES), i32),
            pltpu.VMEM((block_rows, width), BF),
            pltpu.VMEM((block_rows, width), F32),
            pltpu.VMEM((rows, cap, width), BF),
            pltpu.VMEM((rows, cap, width), BF),
            pltpu.VMEM((LANES, width), F32),
            pltpu.VMEM((cols, quarter, width), BF),
            pltpu.VMEM((cols, cols, quarter, width), BF),
            pltpu.VMEM((batch, quarter, d), BF),
            pltpu.VMEM((2, quarter, d), BF),
            pltpu.VMEM(w_qkv.shape, BF),
            pltpu.VMEM(w_out.shape, BF),
            pltpu.VMEM(w_in.shape, BF),
            pltpu.VMEM(w_down.shape, BF),
            pltpu.VMEM((d, d), BF),
            pltpu.VMEM((d, d), BF),
            pltpu.VMEM((2, HEADS, 4 * head_dim, quarter), BF),
            pltpu.VMEM((cols, quarter, 2 * d), BF),
            pltpu.VMEM((cols, d, quarter), BF),
            pltpu.VMEM((2, HEADS, 1, quarter), F32),
            pltpu.VMEM((2, HEADS, 1, quarter), F32),
            pltpu.VMEM((2, HEADS, head_dim, quarter), F32),
            pltpu.VMEM((2, quarter, quarter), F32),
            dma((cols,)),
            dma((cols,)),
            dma((rows,)),
            dma((rows,)),
            dma((rows,)),
            dma((rows,)),
            dma((4,)),
            dma((2,)),
            dma((2, cols)),
            dma((cols, cols)),
            dma((cols, cols)),
            dma((2,)),
            dma((batch,)),
            dma((4,)),
        ],
        compiler_params=pltpu.CompilerParams(
            collective_id=0, has_side_effects=True, vmem_limit_bytes=63 * 1024 * 1024
        ),
    )(token_ids, lengths, table, gain1.reshape(1, d), gain2.reshape(1, d), w_qkv, w_out, w_in, w_down)


def local(token_ids, lengths, table, attn_gain, w_qkv, w_out, mlp_gain, w_in, w_down):
    batch_dev, quarter = token_ids.shape
    col_count = lax.axis_size("cols")
    row_count = lax.axis_size("rows")
    token_count = batch_dev * quarter * col_count
    capacity = -(-(8 * token_count // (3 * row_count)) // 32) * 32
    return whole_call(
        row_count, col_count, capacity, token_ids, lengths, table,
        attn_gain, mlp_gain, w_qkv, w_out, w_in, w_down,
    )


def solution(mesh):
    in_specs = (P("rows", "cols"), P("rows"), P("rows", "cols"), P(), P(), P(), P(), P(), P())
    out_specs = P("rows", "cols", None)
    return jax.shard_map(local, mesh=mesh, in_specs=in_specs, out_specs=out_specs, check_vma=False)
```

```python
import functools

import jax
import jax.numpy as jnp
from jax import lax
from jax.experimental import pallas as pl
from jax.experimental.pallas import tpu as pltpu
from jax.sharding import PartitionSpec as P

HEADS = 8
LANES = 128
NEG = -1e30
SCORE_SCALE = 0.125 * 1.4426950408889634
MESH = pl.DeviceIdType.MESH
BF = jnp.bfloat16
F32 = jnp.float32


def rms_norm(values_f32, gain):
    mean_sq = jnp.mean(values_f32 * values_f32, axis=-1, keepdims=True)
    return values_f32 * lax.rsqrt(mean_sq + 1e-06) * gain


def whole_kernel(
    rows, cols, cap, ids_ref, lens_ref, table_ref, gain1, gain2, wqkv_h, wo_h, wi_h, wd_h, out_ref,
    ids_all, ids_s, slots_v, slots_s, left, right, req, asked, asked_s, tab, wide_tab, outbox, raw,
    stage, ebox, ebuf, hbuf, hstage, wqkv, wo, wi, wd, wq, wv, qm, k_s, v_s, m_s, l_s, acc, s_buf, out_v, normed_s,
    ids_send, ids_recv, req_send, req_recv, row_send, row_recv, tab_sem, smem_sem,
    send_sem, pass_sem, recv_sem, hsend_sem, hrecv_sem, w_sem, out_sem,
):
    me = lax.axis_index("cols")
    mr = lax.axis_index("rows")
    batch, quarter = ids_ref.shape
    block_rows, width = table_ref.shape
    d = width * cols
    tiles = quarter // LANES
    lines = ids_s.shape[0]
    groups = req.shape[1]
    pieces = tab_sem.shape[0]
    piece = block_rows // pieces
    shift = block_rows.bit_length() - 1
    half = quarter // 2
    head_dim = LANES // 2
    group = cols // batch
    hist = me // group
    other = batch - 1 - hist
    inner = group - 1 + hist
    far_inner = group - 1 + other
    mate = hist * group + (group - 1 - lax.rem(me, group))
    is_inner = me == inner
    falling = hist == 0
    hi = jnp.where(is_inner, cols - 1, 0)
    mate_hi = cols - 1 - hi

    def query_of(slot):
        rising = jnp.where(slot == 0, cols - 1, slot)
        for_inner = jnp.where(falling, cols - 1 - slot, rising)
        return jnp.where(is_inner, for_inner, -slot)

    def tab_copy(i):
        part = pl.ds(i * piece, piece)
        return pltpu.make_async_copy(table_ref.at[part], tab.at[part], tab_sem.at[i])

    for i in range(pieces):
        tab_copy(i).start()
    loads = [
        pltpu.make_async_copy(src, dst, w_sem.at[i])
        for i, (src, dst) in enumerate(((wqkv_h, wqkv), (wo_h, wo), (wi_h, wi), (wd_h, wd)))
    ]

    def order(t):
        return jnp.where(t == 0, cols - 1, t - 1)

    def far_copy(j):
        return pltpu.make_async_remote_copy(
            src_ref=ebox.at[j],
            dst_ref=ebuf.at[me, j],
            send_sem=send_sem.at[0, j],
            recv_sem=recv_sem.at[me, j],
            device_id={"cols": far_inner},
            device_id_type=MESH,
        )

    def mate_copy(j):
        return pltpu.make_async_remote_copy(
            src_ref=ebuf.at[me, j],
            dst_ref=ebuf.at[me, j],
            send_sem=send_sem.at[1, j],
            recv_sem=recv_sem.at[me, j],
            device_id={"cols": mate},
            device_id_type=MESH,
        )

    def pass_copy(s, j):
        return pltpu.make_async_remote_copy(
            src_ref=ebuf.at[s, j],
            dst_ref=ebuf.at[s, j],
            send_sem=pass_sem.at[s, j],
            recv_sem=recv_sem.at[s, j],
            device_id={"cols": mate},
            device_id_type=MESH,
        )

    def hidden_copy(slot, p):
        part = pl.ds(p * half, half)
        return pltpu.make_async_remote_copy(
            src_ref=hstage.at[slot, part],
            dst_ref=hbuf.at[hist, part],
            send_sem=hsend_sem.at[slot, p],
            recv_sem=hrecv_sem.at[hist, p],
            device_id={"cols": query_of(slot)},
            device_id_type=MESH,
        )

    def hidden_arrival(h, p):
        part = pl.ds(pl.multiple_of(p * half, half), half)
        return pltpu.make_async_remote_copy(
            src_ref=hstage.at[0, part],
            dst_ref=hbuf.at[h, part],
            send_sem=hsend_sem.at[0, p],
            recv_sem=hrecv_sem.at[h, p],
            device_id={"cols": mate},
            device_id_type=MESH,
        )

    def ids_copy(c):
        return pltpu.make_async_remote_copy(
            src_ref=ids_ref,
            dst_ref=ids_all.at[me],
            send_sem=ids_send.at[c],
            recv_sem=ids_recv.at[me],
            device_id={"cols": c},
            device_id_type=MESH,
        )

    def ids_arrival(c):
        return pltpu.make_async_remote_copy(
            src_ref=ids_ref,
            dst_ref=ids_all.at[c],
            send_sem=ids_send.at[c],
            recv_sem=ids_recv.at[c],
            device_id={"cols": c},
            device_id_type=MESH,
        )

    def req_copy(r):
        return pltpu.make_async_remote_copy(
            src_ref=req.at[r],
            dst_ref=asked.at[mr],
            send_sem=req_send.at[r],
            recv_sem=req_recv.at[mr],
            device_id={"rows": r},
            device_id_type=MESH,
        )

    def req_arrival(r):
        return pltpu.make_async_remote_copy(
            src_ref=req.at[r],
            dst_ref=asked.at[r],
            send_sem=req_send.at[r],
            recv_sem=req_recv.at[r],
            device_id={"rows": r},
            device_id_type=MESH,
        )

    front = cap // LANES // 2 * LANES
    spans = (pl.ds(0, front), pl.ds(front, cap - front))

    def row_copy(r, p):
        return pltpu.make_async_remote_copy(
            src_ref=outbox.at[r, spans[p]],
            dst_ref=raw.at[mr, spans[p]],
            send_sem=row_send.at[r, p],
            recv_sem=row_recv.at[mr, p],
            device_id={"rows": r},
            device_id_type=MESH,
        )

    def row_arrival(r, p):
        return pltpu.make_async_remote_copy(
            src_ref=outbox.at[r, spans[p]],
            dst_ref=raw.at[r, spans[p]],
            send_sem=row_send.at[r, p],
            recv_sem=row_recv.at[r, p],
            device_id={"rows": r},
            device_id_type=MESH,
        )

    barrier = pltpu.get_barrier_semaphore()
    for off in range(1, cols):
        pl.semaphore_signal(
            barrier, inc=1, device_id={"cols": lax.rem(me + off, cols)}, device_id_type=MESH
        )
    for off in range(1, rows):
        pl.semaphore_signal(
            barrier, inc=1, device_id={"rows": lax.rem(mr + off, rows)}, device_id_type=MESH
        )
    pl.semaphore_wait(barrier, cols - 1 + rows - 1)

    for off in range(1, cols):
        ids_copy(lax.rem(me + off, cols)).start()
    for load in loads:
        load.start()
    ids_all[me] = ids_ref[...]

    step = 512
    for i in range(pieces):
        tab_copy(i).wait()

        def widen(k, carry):
            part = pl.ds(pl.multiple_of(i * piece + k * step, step), step)
            wide_tab[part, :] = tab[part, :].astype(F32)
            return carry

        lax.fori_loop(0, piece // step, widen, 0)

    for off in range(1, cols):
        ids_arrival(lax.rem(me + off, cols)).wait_recv()
    for c in range(cols):
        for b in range(batch):
            for k in range(tiles):
                line = (c * batch + b) * tiles + k
                ids_s[line : line + 1, :] = ids_all[c, b : b + 1, k * LANES : (k + 1) * LANES]
    ids = ids_s[...]
    owner = lax.shift_right_logical(ids, shift)
    offset = ids - owner * block_rows

    src_lane = lax.broadcasted_iota(jnp.int32, (LANES, 2 * LANES), 0)
    dst_lane = lax.broadcasted_iota(jnp.int32, (LANES, 2 * LANES), 1)
    before = jnp.where(src_lane < dst_lane, 1.0, 0.0).astype(BF)
    line_a = lax.broadcasted_iota(jnp.int32, (lines, lines), 0)
    line_b = lax.broadcasted_iota(jnp.int32, (lines, lines), 1)
    above = jnp.where(line_b < line_a, 1.0, 0.0).astype(BF)
    rank = jnp.zeros((lines, LANES), F32)
    for r in range(rows):
        mine = owner == r
        counts = jnp.dot(
            jnp.where(mine, 1.0, 0.0).astype(BF), before, preferred_element_type=F32
        )
        earlier = jnp.dot(above, counts[:, LANES:].astype(BF), preferred_element_type=F32)
        rank = rank + jnp.where(mine, counts[:, :LANES] + earlier, 0.0)
    rank = rank.astype(jnp.int32)
    slots_v[...] = jnp.minimum(jnp.maximum(owner * cap + rank, 0), rows * cap - 1)
    slot_group = owner * groups + lax.shift_right_logical(rank, 7)
    lane = rank - lax.shift_right_logical(rank, 7) * LANES
    high = lax.shift_right_logical(offset, 7)
    low_part = (offset - high * LANES).astype(F32)
    high = high.astype(F32)
    group_iota = lax.broadcasted_iota(jnp.int32, (rows * groups, LANES), 0)
    lane_iota = lax.broadcasted_iota(jnp.int32, (LANES, LANES), 0)
    for k in range(lines):
        part = slice(k * LANES, (k + 1) * LANES)
        line = slice(k, k + 1)
        left[:, part] = jnp.where(slot_group[line] == group_iota, 1.0, 0.0).astype(BF)
        hit = lane[line] == lane_iota
        right[:LANES, part] = jnp.where(hit, high[line], 0.0).astype(BF)
        right[LANES:, part] = jnp.where(hit, low_part[line], 0.0).astype(BF)
    found = lax.dot_general(
        left[...], right[...], (((1,), (1,)), ((), ())), preferred_element_type=F32
    )
    found = (found[:, :LANES] * LANES + found[:, LANES:]).astype(jnp.int32)
    found = jnp.minimum(jnp.maximum(found, 0), block_rows - 1)
    req[...] = found.reshape(rows, groups, LANES)

    def offset_of(i):
        return rows // 2 + (i + 1) // 2 * (1 - 2 * lax.rem(i, 2))

    def over_rows(act):
        def body(i, carry):
            act(lax.rem(mr + i + 1, rows))
            return carry

        lax.fori_loop(0, rows - 1, body, 0)

    over_rows(lambda r: req_copy(r).start())
    asked[mr] = req[mr]
    slots_copy = pltpu.make_async_copy(slots_v, slots_s, smem_sem.at[1])
    slots_copy.start()

    def some(r, g, count):
        for u in range(count):
            stage[u : u + 1, :] = wide_tab[pl.ds(asked_s[r, g, u], 1), :]
        part = pl.ds(pl.multiple_of(g * LANES, LANES), count)
        outbox[r, part, :] = stage[:count].astype(BF)

    def serve(i, carry):
        back = i // rows
        i = lax.rem(i, rows)
        r = lax.rem(mr + offset_of(i), rows)

        @pl.when(back == 0)
        def _():
            @pl.when(i < rows - 1)
            def _():
                req_arrival(r).wait_recv()

            to_smem = pltpu.make_async_copy(asked.at[r], asked_s.at[r], smem_sem.at[0])
            to_smem.start()
            to_smem.wait()

        def full_line(g, carry):
            some(r, g, LANES)
            return carry

        line_from = jnp.where(back == 0, 0, front // LANES)
        line_to = jnp.where(back == 0, front // LANES, cap // LANES)
        lax.fori_loop(line_from, line_to, full_line, 0)

        @pl.when((back == 0) & (i < rows - 1))
        def _():
            row_copy(r, 0).start()

        @pl.when(back == 1)
        def _():
            if cap % LANES:
                some(r, cap // LANES, cap % LANES)

            @pl.when(i < rows - 1)
            def _():
                row_copy(r, 1).start()

        return carry

    lax.fori_loop(0, 2 * rows, serve, 0)

    loads[0].wait()
    wq[...] = wqkv[:, :d].astype(F32).T.astype(BF)
    wv[...] = wqkv[:, 2 * d :].astype(F32).T.astype(BF)
    for load in loads[1:]:
        load.wait()

    def widen_row(i, carry):
        r = lax.rem(mr + rows - offset_of(i), rows)
        part = pl.ds(pl.multiple_of(r * cap, 16), cap)

        @pl.when(i < rows - 1)
        def _():
            for p in range(2):
                row_arrival(r, p).wait_recv()
            wide_tab[part, :] = raw[r].astype(F32)

        @pl.when(i == rows - 1)
        def _():
            wide_tab[part, :] = outbox[r].astype(F32)

        return carry

    slots_copy.wait()
    lax.fori_loop(0, rows, widen_row, 0)


    def pick(t, carry):
        for side in range(2):
            h = other if side == 0 else hist
            j = order(t)
            line = (j * batch + h) * tiles
            for k in range(tiles):
                for u in range(LANES):
                    stage[u : u + 1, :] = wide_tab[pl.ds(slots_s[line + k, u], 1), :]
                part = slice(k * LANES, (k + 1) * LANES)
                if side == 0:
                    ebox[j, part, :] = stage[...].astype(BF)
                else:
                    ebuf[me, j, part, :] = stage[...].astype(BF)
            if side == 0:
                far_copy(j).start()
            else:

                @pl.when(j <= mate_hi)
                def _():
                    mate_copy(j).start()

        return carry

    lax.fori_loop(0, cols, pick, 0)
    dims_nt = (((1,), (1,)), ((), ()))
    length = lens_ref[hist]

    def embedded(j):
        parts = [ebuf[s, j] for s in range(cols)]
        return jnp.concatenate(parts, axis=1).astype(F32)

    def attend(slot, j, causal):
        if causal:
            items = [(h, n, n - half, half) for h in range(HEADS) for n in (half, quarter)]
        else:
            items = [(h, quarter, 0, quarter) for h in range(HEADS)]

        def scores(at):
            h, kn, q0, qn = items[at]
            k_blk = k_s[j, :kn, (h // 2) * 2 * LANES : (h // 2 + 1) * 2 * LANES]
            s = jnp.dot(k_blk, qm[slot, h, :, q0 : q0 + qn], preferred_element_type=F32)
            if causal:
                key_pos = lax.broadcasted_iota(jnp.int32, (kn, qn), 0)
                query_pos = lax.broadcasted_iota(jnp.int32, (kn, qn), 1) + q0
                s = jnp.where(key_pos <= query_pos, s, NEG)
            s_buf[at % 2, :kn, :qn] = s
            return jnp.max(s, axis=0, keepdims=True)

        top = scores(0)
        for at, (h, kn, q0, qn) in enumerate(items):
            next_top = scores(at + 1) if at + 1 < len(items) else None
            cut = slice(q0, q0 + qn)
            m_old = m_s[slot, h, :, cut]
            m_new = jnp.maximum(m_old, top)
            probs = jnp.exp2(s_buf[at % 2, :kn, :qn] - m_new)
            alpha = jnp.exp2(m_old - m_new)
            m_s[slot, h, :, cut] = m_new
            l_s[slot, h, :, cut] = l_s[slot, h, :, cut] * alpha + jnp.sum(
                probs, axis=0, keepdims=True
            )
            v_t = v_s[j, h * head_dim : (h + 1) * head_dim, :kn]
            acc[slot, h, :, cut] = acc[slot, h, :, cut] * alpha + jnp.dot(
                v_t, probs.astype(BF), preferred_element_type=F32
            )
            top = next_top

    def arrive(j):
        for s in range(cols):
            far = s // group == other

            @pl.when((s != me) & (j <= hi))
            def _():
                pass_copy(s, j).wait_recv()

            @pl.when(is_inner & far & (j == 0))
            def _():
                pass_copy(s, j).start()

    def project(j):
        normed = rms_norm(embedded(j), gain1[...]).astype(BF)
        normed_s[...] = normed
        keys = jnp.dot(normed, wqkv[:, d : 2 * d], preferred_element_type=F32).astype(BF)
        row = lax.broadcasted_iota(jnp.int32, (quarter, LANES), 0)
        lane = lax.broadcasted_iota(jnp.int32, (quarter, LANES), 1)
        dead = (lane == 0) & (row >= length - j * quarter)
        bias = jnp.where(dead, NEG, 0.0).astype(BF)
        for p in range(HEADS // 2):
            k_s[j, :, 2 * p * LANES : (2 * p + 1) * LANES] = keys[:, p * LANES : (p + 1) * LANES]
            k_s[j, :, (2 * p + 1) * LANES : (2 * p + 2) * LANES] = bias
        v_s[j] = lax.dot_general(wv[...], normed, dims_nt, preferred_element_type=F32).astype(BF)


    def queries(slot):
        q_t = lax.dot_general(wq[...], normed_s[...], dims_nt, preferred_element_type=F32)
        q_t = (q_t * SCORE_SCALE).astype(BF)
        zero = jnp.zeros((head_dim, quarter), BF)
        one_row = lax.broadcasted_iota(jnp.int32, (LANES, quarter), 0) == 0
        one_row = jnp.where(one_row, 1.0, 0.0).astype(BF)
        for h in range(HEADS):
            mine = q_t[h * head_dim : (h + 1) * head_dim]
            pair = (mine, zero) if h % 2 == 0 else (zero, mine)
            qm[slot, h] = jnp.concatenate(pair + (one_row,), axis=0)
        m_s[slot] = jnp.full(m_s.shape[1:], NEG, F32)
        l_s[slot] = jnp.zeros(l_s.shape[1:], F32)
        acc[slot] = jnp.zeros(acc.shape[1:], F32)

    def step(t, carry):
        j = order(t)

        @pl.when(j <= hi)
        def _():
            arrive(j)
            project(j)

        def query_step(slot, carry):
            q = query_of(slot)
            @pl.when(j == q)
            def _():
                queries(slot)

            top_q = q == cols - 1
            late = falling & is_inner & (slot == 2)
            ready = jnp.where(late, t == cols - 1, j == q)
            fresh = jnp.where(top_q, 1, q + 1)
            count = jnp.where(ready, fresh, jnp.where(top_q & (j < q), 1, 0))
            first = jnp.where(late, q, j)
            done = jnp.where(top_q, t == cols - 1, ready)

            def unit(i, carry):
                key = first - i

                @pl.when(key == q)
                def _():
                    attend(slot, key, True)

                @pl.when(key < q)
                def _():
                    attend(slot, key, False)

                return carry

            lax.fori_loop(0, count, unit, 0)

            @pl.when(done)
            def _():
                for p in range(2):
                    cut = slice(p * half, (p + 1) * half)
                    att_t = acc[slot, :, :, cut] / l_s[slot, :, :, cut]
                    attended = att_t.reshape(HEADS * head_dim, half).T.astype(BF)
                    rows_in = [ebuf[s, q, cut] for s in range(cols)]
                    hidden = jnp.concatenate(rows_in, axis=1).astype(F32) + jnp.dot(
                        attended, wo[...], preferred_element_type=F32
                    )
                    hidden = hidden.astype(BF)

                    @pl.when(q == me)
                    def _():
                        hbuf[hist, cut] = hidden

                    @pl.when(q != me)
                    def _():
                        hstage[slot, cut] = hidden
                        hidden_copy(slot, p).start()

            return carry

        @pl.when(j <= hi)
        def _():
            lax.fori_loop(0, 3, query_step, 0)

        return carry

    lax.fori_loop(0, cols, step, 0)

    def mlp(i, carry):
        first = jnp.where(falling | is_inner, hist, other)
        h = jnp.where(i < 2, first, batch - 1 - first)
        p = lax.rem(i, 2)
        part = pl.ds(pl.multiple_of(p * half, half), half)

        local = (query_of(0) == me) | (query_of(1) == me) | (query_of(2) == me)

        @pl.when((h != hist) | ~local)
        def _():
            hidden_arrival(h, p).wait_recv()

        hidden = hbuf[h, part, :].astype(F32)
        normed_two = rms_norm(hidden, gain2[...]).astype(BF)
        ff = wd.shape[0]
        tile = 512
        total = hidden
        for f in range(0, ff, tile):
            gate = jnp.dot(normed_two, wi[:, f : f + tile], preferred_element_type=F32)
            up = jnp.dot(normed_two, wi[:, ff + f : ff + f + tile], preferred_element_type=F32)
            act = (gate / (1.0 + jnp.exp(-gate)) * up).astype(BF)
            total = total + jnp.dot(act, wd[f : f + tile, :], preferred_element_type=F32)
        out_v[i] = total.astype(BF)
        out_copy(i).start()
        return carry

    def out_copy(i):
        first = jnp.where(falling | is_inner, hist, other)
        h = jnp.where(i < 2, first, batch - 1 - first)
        part = pl.ds(pl.multiple_of(lax.rem(i, 2) * half, half), half)
        return pltpu.make_async_copy(out_v.at[i], out_ref.at[h, part], out_sem.at[i])

    lax.fori_loop(0, 2 * batch, mlp, 0)
    for i in range(2 * batch):
        out_copy(i).wait()
    for j in range(cols):
        far_copy(j).wait_send()

        @pl.when(j <= mate_hi)
        def _():
            mate_copy(j).wait_send()

        for s in range(cols):

            @pl.when(is_inner & (s // group == other) & (j == 0))
            def _():
                pass_copy(s, j).wait_send()

    for slot in range(3):

        @pl.when((query_of(slot) != me) & (query_of(slot) >= 0))
        def _():
            for p in range(2):
                hidden_copy(slot, p).wait_send()

    for off in range(1, cols):
        ids_copy(lax.rem(me + off, cols)).wait_send()
    over_rows(lambda r: req_copy(r).wait_send())
    for p in range(2):
        over_rows(lambda r: row_copy(r, p).wait_send())


def whole_call(rows, cols, cap, token_ids, lengths, table, gain1, gain2, w_qkv, w_out, w_in, w_down):
    batch, quarter = token_ids.shape
    tokens = batch * quarter * cols
    lines = tokens // LANES
    block_rows, width = table.shape
    d = width * cols
    head_dim = d // HEADS
    assert batch == 2 and cols == 2 * batch and rows % 2 == 0
    assert block_rows & (block_rows - 1) == 0 and rows * cap <= block_rows
    groups = -(-cap // (8 * LANES)) * 8
    any_spec = pl.BlockSpec(memory_space=pl.ANY)
    vmem = pl.BlockSpec(memory_space=pltpu.VMEM)
    smem = pl.BlockSpec(memory_space=pltpu.SMEM)
    dma = pltpu.SemaphoreType.DMA
    i32 = jnp.int32
    return pl.pallas_call(
        functools.partial(whole_kernel, rows, cols, cap),
        out_shape=jax.ShapeDtypeStruct((batch, quarter, d), BF),
        in_specs=[vmem, smem, any_spec, vmem, vmem] + [any_spec] * 4,
        out_specs=any_spec,
        scratch_shapes=[
            pltpu.VMEM((cols, batch, quarter), i32),
            pltpu.VMEM((lines, LANES), i32),
            pltpu.VMEM((lines, LANES), i32),
            pltpu.SMEM((lines, LANES), i32),
            pltpu.VMEM((rows * groups, tokens), BF),
            pltpu.VMEM((2 * LANES, tokens), BF),
            pltpu.VMEM((rows, groups, LANES), i32),
            pltpu.VMEM((rows, groups, LANES), i32),
            pltpu.SMEM((rows, groups, LANES), i32),
            pltpu.VMEM((block_rows, width), BF),
            pltpu.VMEM((block_rows, width), F32),
            pltpu.VMEM((rows, cap, width), BF),
            pltpu.VMEM((rows, cap, width), BF),
            pltpu.VMEM((LANES, width), F32),
            pltpu.VMEM((cols, quarter, width), BF),
            pltpu.VMEM((cols, cols, quarter, width), BF),
            pltpu.VMEM((batch, quarter, d), BF),
            pltpu.VMEM((3, quarter, d), BF),
            pltpu.VMEM(w_qkv.shape, BF),
            pltpu.VMEM(w_out.shape, BF),
            pltpu.VMEM(w_in.shape, BF),
            pltpu.VMEM(w_down.shape, BF),
            pltpu.VMEM((d, d), BF),
            pltpu.VMEM((d, d), BF),
            pltpu.VMEM((3, HEADS, 4 * head_dim, quarter), BF),
            pltpu.VMEM((cols, quarter, 2 * d), BF),
            pltpu.VMEM((cols, d, quarter), BF),
            pltpu.VMEM((3, HEADS, 1, quarter), F32),
            pltpu.VMEM((3, HEADS, 1, quarter), F32),
            pltpu.VMEM((3, HEADS, head_dim, quarter), F32),
            pltpu.VMEM((2, quarter, quarter), F32),
            pltpu.VMEM((2 * batch, quarter // 2, d), BF),
            pltpu.VMEM((quarter, d), BF),
            dma((cols,)),
            dma((cols,)),
            dma((rows,)),
            dma((rows,)),
            dma((rows, 2)),
            dma((rows, 2)),
            dma((4,)),
            dma((2,)),
            dma((2, cols)),
            dma((cols, cols)),
            dma((cols, cols)),
            dma((3, 2)),
            dma((batch, 2)),
            dma((4,)),
            dma((2 * batch,)),
        ],
        compiler_params=pltpu.CompilerParams(
            collective_id=0, has_side_effects=True, vmem_limit_bytes=63 * 1024 * 1024
        ),
    )(token_ids, lengths, table, gain1.reshape(1, d), gain2.reshape(1, d), w_qkv, w_out, w_in, w_down)


def local(token_ids, lengths, table, attn_gain, w_qkv, w_out, mlp_gain, w_in, w_down):
    batch_dev, quarter = token_ids.shape
    col_count = lax.axis_size("cols")
    row_count = lax.axis_size("rows")
    token_count = batch_dev * quarter * col_count
    capacity = -(-(8 * token_count // (3 * row_count)) // 32) * 32
    return whole_call(
        row_count, col_count, capacity, token_ids, lengths, table,
        attn_gain, mlp_gain, w_qkv, w_out, w_in, w_down,
    )


def solution(mesh):
    in_specs = (P("rows", "cols"), P("rows"), P("rows", "cols"), P(), P(), P(), P(), P(), P())
    out_specs = P("rows", "cols", None)
    return jax.shard_map(local, mesh=mesh, in_specs=in_specs, out_specs=out_specs, check_vma=False)
```

```python
import functools

import jax
import jax.numpy as jnp
from jax import lax
from jax.experimental import pallas as pl
from jax.experimental.pallas import tpu as pltpu
from jax.sharding import PartitionSpec as P

HEADS = 8
LANES = 128
NEG = -1e30
SCORE_SCALE = 0.125 * 1.4426950408889634
MESH = pl.DeviceIdType.MESH
BF = jnp.bfloat16
F32 = jnp.float32


def rms_norm(values_f32, gain):
    mean_sq = jnp.mean(values_f32 * values_f32, axis=-1, keepdims=True)
    return values_f32 * lax.rsqrt(mean_sq + 1e-06) * gain


def whole_kernel(
    rows, cols, cap, ids_ref, lens_ref, table_ref, gain1, gain2, wqkv_h, wo_h, wi_h, wd_h, out_ref,
    ids_all, ids_s, slots_v, slots_s, left, right, req, asked, asked_s, tab, wide_tab, outbox, raw,
    stage, ebox, ebuf, hbuf, hstage, wqkv, wo, wi, wd, wq, wv, qm, k_s, v_s, m_s, l_s, acc, s_buf, out_v, normed_s,
    ids_send, ids_recv, req_send, req_recv, row_send, row_recv, tab_sem, smem_sem,
    send_sem, pass_sem, recv_sem, hsend_sem, hrecv_sem, w_sem, out_sem,
):
    me = lax.axis_index("cols")
    mr = lax.axis_index("rows")
    batch, quarter = ids_ref.shape
    block_rows, width = table_ref.shape
    d = width * cols
    tiles = quarter // LANES
    lines = ids_s.shape[0]
    groups = req.shape[1]
    pieces = tab_sem.shape[0]
    piece = block_rows // pieces
    shift = block_rows.bit_length() - 1
    half = quarter // 2
    head_dim = LANES // 2
    group = cols // batch
    hist = me // group
    other = batch - 1 - hist
    inner = group - 1 + hist
    far_inner = group - 1 + other
    mate = hist * group + (group - 1 - lax.rem(me, group))
    is_inner = me == inner
    falling = hist == 0
    hi = jnp.where(is_inner, cols - 1, 0)
    mate_hi = cols - 1 - hi

    def query_of(slot):
        rising = jnp.where(slot == 0, cols - 1, slot)
        for_inner = jnp.where(falling, cols - 1 - slot, rising)
        return jnp.where(is_inner, for_inner, -slot)

    def tab_copy(i):
        part = pl.ds(i * piece, piece)
        return pltpu.make_async_copy(table_ref.at[part], tab.at[part], tab_sem.at[i])

    for i in range(pieces):
        tab_copy(i).start()
    loads = [
        pltpu.make_async_copy(src, dst, w_sem.at[i])
        for i, (src, dst) in enumerate(((wqkv_h, wqkv), (wo_h, wo), (wi_h, wi), (wd_h, wd)))
    ]

    def order(t):
        return jnp.where(t == 0, cols - 1, t - 1)

    def far_copy(j):
        return pltpu.make_async_remote_copy(
            src_ref=ebox.at[j],
            dst_ref=ebuf.at[me, j],
            send_sem=send_sem.at[0, j],
            recv_sem=recv_sem.at[me, j],
            device_id={"cols": far_inner},
            device_id_type=MESH,
        )

    def mate_copy(j):
        return pltpu.make_async_remote_copy(
            src_ref=ebuf.at[me, j],
            dst_ref=ebuf.at[me, j],
            send_sem=send_sem.at[1, j],
            recv_sem=recv_sem.at[me, j],
            device_id={"cols": mate},
            device_id_type=MESH,
        )

    def pass_copy(s, j):
        return pltpu.make_async_remote_copy(
            src_ref=ebuf.at[s, j],
            dst_ref=ebuf.at[s, j],
            send_sem=pass_sem.at[s, j],
            recv_sem=recv_sem.at[s, j],
            device_id={"cols": mate},
            device_id_type=MESH,
        )

    def hidden_copy(slot, p):
        part = pl.ds(p * half, half)
        return pltpu.make_async_remote_copy(
            src_ref=hstage.at[slot, part],
            dst_ref=hbuf.at[hist, part],
            send_sem=hsend_sem.at[slot, p],
            recv_sem=hrecv_sem.at[hist, p],
            device_id={"cols": query_of(slot)},
            device_id_type=MESH,
        )

    def hidden_arrival(h, p):
        part = pl.ds(pl.multiple_of(p * half, half), half)
        return pltpu.make_async_remote_copy(
            src_ref=hstage.at[0, part],
            dst_ref=hbuf.at[h, part],
            send_sem=hsend_sem.at[0, p],
            recv_sem=hrecv_sem.at[h, p],
            device_id={"cols": mate},
            device_id_type=MESH,
        )

    def ids_copy(c):
        return pltpu.make_async_remote_copy(
            src_ref=ids_ref,
            dst_ref=ids_all.at[me],
            send_sem=ids_send.at[c],
            recv_sem=ids_recv.at[me],
            device_id={"cols": c},
            device_id_type=MESH,
        )

    def ids_arrival(c):
        return pltpu.make_async_remote_copy(
            src_ref=ids_ref,
            dst_ref=ids_all.at[c],
            send_sem=ids_send.at[c],
            recv_sem=ids_recv.at[c],
            device_id={"cols": c},
            device_id_type=MESH,
        )

    def req_copy(r):
        return pltpu.make_async_remote_copy(
            src_ref=req.at[r],
            dst_ref=asked.at[mr],
            send_sem=req_send.at[r],
            recv_sem=req_recv.at[mr],
            device_id={"rows": r},
            device_id_type=MESH,
        )

    def req_arrival(r):
        return pltpu.make_async_remote_copy(
            src_ref=req.at[r],
            dst_ref=asked.at[r],
            send_sem=req_send.at[r],
            recv_sem=req_recv.at[r],
            device_id={"rows": r},
            device_id_type=MESH,
        )

    front = cap // LANES // 2 * LANES
    spans = (pl.ds(0, front), pl.ds(front, cap - front))

    def row_copy(r, p):
        return pltpu.make_async_remote_copy(
            src_ref=outbox.at[r, spans[p]],
            dst_ref=raw.at[mr, spans[p]],
            send_sem=row_send.at[r, p],
            recv_sem=row_recv.at[mr, p],
            device_id={"rows": r},
            device_id_type=MESH,
        )

    def row_arrival(r, p):
        return pltpu.make_async_remote_copy(
            src_ref=outbox.at[r, spans[p]],
            dst_ref=raw.at[r, spans[p]],
            send_sem=row_send.at[r, p],
            recv_sem=row_recv.at[r, p],
            device_id={"rows": r},
            device_id_type=MESH,
        )

    barrier = pltpu.get_barrier_semaphore()
    for off in range(1, cols):
        pl.semaphore_signal(
            barrier, inc=1, device_id={"cols": lax.rem(me + off, cols)}, device_id_type=MESH
        )
    for off in range(1, rows):
        pl.semaphore_signal(
            barrier, inc=1, device_id={"rows": lax.rem(mr + off, rows)}, device_id_type=MESH
        )
    pl.semaphore_wait(barrier, cols - 1 + rows - 1)

    for off in range(1, cols):
        ids_copy(lax.rem(me + off, cols)).start()
    for load in loads:
        load.start()
    ids_all[me] = ids_ref[...]

    step = 512
    for i in range(pieces):
        tab_copy(i).wait()

        def widen(k, carry):
            part = pl.ds(pl.multiple_of(i * piece + k * step, step), step)
            wide_tab[part, :] = tab[part, :].astype(F32)
            return carry

        lax.fori_loop(0, piece // step, widen, 0)

    for off in range(1, cols):
        ids_arrival(lax.rem(me + off, cols)).wait_recv()
    for c in range(cols):
        for b in range(batch):
            for k in range(tiles):
                line = (c * batch + b) * tiles + k
                ids_s[line : line + 1, :] = ids_all[c, b : b + 1, k * LANES : (k + 1) * LANES]
    ids = ids_s[...]
    owner = lax.shift_right_logical(ids, shift)
    offset = ids - owner * block_rows

    src_lane = lax.broadcasted_iota(jnp.int32, (LANES, 2 * LANES), 0)
    dst_lane = lax.broadcasted_iota(jnp.int32, (LANES, 2 * LANES), 1)
    before = jnp.where(src_lane < dst_lane, 1.0, 0.0).astype(BF)
    line_a = lax.broadcasted_iota(jnp.int32, (lines, lines), 0)
    line_b = lax.broadcasted_iota(jnp.int32, (lines, lines), 1)
    above = jnp.where(line_b < line_a, 1.0, 0.0).astype(BF)
    rank = jnp.zeros((lines, LANES), F32)
    for r in range(rows):
        mine = owner == r
        counts = jnp.dot(
            jnp.where(mine, 1.0, 0.0).astype(BF), before, preferred_element_type=F32
        )
        earlier = jnp.dot(above, counts[:, LANES:].astype(BF), preferred_element_type=F32)
        rank = rank + jnp.where(mine, counts[:, :LANES] + earlier, 0.0)
    rank = rank.astype(jnp.int32)
    slots_v[...] = jnp.minimum(jnp.maximum(owner * cap + rank, 0), rows * cap - 1)
    slot_group = owner * groups + lax.shift_right_logical(rank, 7)
    lane = rank - lax.shift_right_logical(rank, 7) * LANES
    high = lax.shift_right_logical(offset, 7)
    low_part = (offset - high * LANES).astype(F32)
    high = high.astype(F32)
    group_iota = lax.broadcasted_iota(jnp.int32, (rows * groups, LANES), 0)
    lane_iota = lax.broadcasted_iota(jnp.int32, (LANES, LANES), 0)
    for k in range(lines):
        part = slice(k * LANES, (k + 1) * LANES)
        line = slice(k, k + 1)
        left[:, part] = jnp.where(slot_group[line] == group_iota, 1.0, 0.0).astype(BF)
        hit = lane[line] == lane_iota
        right[:LANES, part] = jnp.where(hit, high[line], 0.0).astype(BF)
        right[LANES:, part] = jnp.where(hit, low_part[line], 0.0).astype(BF)
    found = lax.dot_general(
        left[...], right[...], (((1,), (1,)), ((), ())), preferred_element_type=F32
    )
    found = (found[:, :LANES] * LANES + found[:, LANES:]).astype(jnp.int32)
    found = jnp.minimum(jnp.maximum(found, 0), block_rows - 1)
    req[...] = found.reshape(rows, groups, LANES)

    def offset_of(i):
        return rows // 2 + (i + 1) // 2 * (1 - 2 * lax.rem(i, 2))

    def over_rows(act):
        def body(i, carry):
            act(lax.rem(mr + i + 1, rows))
            return carry

        lax.fori_loop(0, rows - 1, body, 0)

    over_rows(lambda r: req_copy(r).start())
    asked[mr] = req[mr]
    slots_copy = pltpu.make_async_copy(slots_v, slots_s, smem_sem.at[1])
    slots_copy.start()

    def some(r, g, count):
        for u in range(count):
            stage[u : u + 1, :] = wide_tab[pl.ds(asked_s[r, g, u], 1), :]
        part = pl.ds(pl.multiple_of(g * LANES, LANES), count)
        outbox[r, part, :] = stage[:count].astype(BF)

    def serve(i, carry):
        back = i // rows
        i = lax.rem(i, rows)
        r = lax.rem(mr + offset_of(i), rows)

        @pl.when(back == 0)
        def _():
            @pl.when(i < rows - 1)
            def _():
                req_arrival(r).wait_recv()

            to_smem = pltpu.make_async_copy(asked.at[r], asked_s.at[r], smem_sem.at[0])
            to_smem.start()
            to_smem.wait()

        def full_line(g, carry):
            some(r, g, LANES)
            return carry

        line_from = jnp.where(back == 0, 0, front // LANES)
        line_to = jnp.where(back == 0, front // LANES, cap // LANES)
        lax.fori_loop(line_from, line_to, full_line, 0)

        @pl.when((back == 0) & (i < rows - 1))
        def _():
            row_copy(r, 0).start()

        @pl.when(back == 1)
        def _():
            if cap % LANES:
                some(r, cap // LANES, cap % LANES)

            @pl.when(i < rows - 1)
            def _():
                row_copy(r, 1).start()

        return carry

    lax.fori_loop(0, 2 * rows, serve, 0)

    loads[0].wait()
    wq[...] = wqkv[:, :d].astype(F32).T.astype(BF)
    wv[...] = wqkv[:, 2 * d :].astype(F32).T.astype(BF)
    for load in loads[1:]:
        load.wait()

    def widen_row(i, carry):
        r = lax.rem(mr + rows - offset_of(i), rows)
        part = pl.ds(pl.multiple_of(r * cap, 16), cap)

        @pl.when(i < rows - 1)
        def _():
            for p in range(2):
                row_arrival(r, p).wait_recv()
            wide_tab[part, :] = raw[r].astype(F32)

        @pl.when(i == rows - 1)
        def _():
            wide_tab[part, :] = outbox[r].astype(F32)

        return carry

    slots_copy.wait()
    lax.fori_loop(0, rows, widen_row, 0)


    def pick(t, carry):
        for side in range(2):
            h = other if side == 0 else hist
            j = order(t)
            line = (j * batch + h) * tiles
            for k in range(tiles):
                for u in range(LANES):
                    stage[u : u + 1, :] = wide_tab[pl.ds(slots_s[line + k, u], 1), :]
                part = slice(k * LANES, (k + 1) * LANES)
                if side == 0:
                    ebox[j, part, :] = stage[...].astype(BF)
                else:
                    ebuf[me, j, part, :] = stage[...].astype(BF)
            if side == 0:
                far_copy(j).start()
            else:

                @pl.when(j <= mate_hi)
                def _():
                    mate_copy(j).start()

        return carry

    lax.fori_loop(0, cols, pick, 0)
    dims_nt = (((1,), (1,)), ((), ()))
    length = lens_ref[hist]

    def embedded(j):
        parts = [ebuf[s, j] for s in range(cols)]
        return jnp.concatenate(parts, axis=1).astype(F32)

    def attend(slot, j, causal):
        if causal:
            items = [(h, n, n - half, half) for h in range(HEADS) for n in (half, quarter)]
        else:
            items = [(h, quarter, 0, quarter) for h in range(HEADS)]

        def scores(at):
            h, kn, q0, qn = items[at]
            k_blk = k_s[j, :kn, (h // 2) * 2 * LANES : (h // 2 + 1) * 2 * LANES]
            s = jnp.dot(k_blk, qm[slot, h, :, q0 : q0 + qn], preferred_element_type=F32)
            if causal:
                key_pos = lax.broadcasted_iota(jnp.int32, (kn, qn), 0)
                query_pos = lax.broadcasted_iota(jnp.int32, (kn, qn), 1) + q0
                s = jnp.where(key_pos <= query_pos, s, NEG)
            s_buf[at % 2, :kn, :qn] = s
            return jnp.max(s, axis=0, keepdims=True)

        top = scores(0)
        for at, (h, kn, q0, qn) in enumerate(items):
            next_top = scores(at + 1) if at + 1 < len(items) else None
            cut = slice(q0, q0 + qn)
            m_old = m_s[slot, h, :, cut]
            m_new = jnp.maximum(m_old, top)
            probs = jnp.exp2(s_buf[at % 2, :kn, :qn] - m_new)
            alpha = jnp.exp2(m_old - m_new)
            m_s[slot, h, :, cut] = m_new
            l_s[slot, h, :, cut] = l_s[slot, h, :, cut] * alpha + jnp.sum(
                probs, axis=0, keepdims=True
            )
            v_t = v_s[j, h * head_dim : (h + 1) * head_dim, :kn]
            acc[slot, h, :, cut] = acc[slot, h, :, cut] * alpha + jnp.dot(
                v_t, probs.astype(BF), preferred_element_type=F32
            )
            top = next_top

    def arrive(j):
        for s in range(cols):
            far = s // group == other

            @pl.when((s != me) & (j <= hi))
            def _():
                pass_copy(s, j).wait_recv()

            @pl.when(is_inner & far & (j == 0))
            def _():
                pass_copy(s, j).start()

    def project(j):
        normed = rms_norm(embedded(j), gain1[...]).astype(BF)
        normed_s[...] = normed
        keys = jnp.dot(normed, wqkv[:, d : 2 * d], preferred_element_type=F32).astype(BF)
        row = lax.broadcasted_iota(jnp.int32, (quarter, LANES), 0)
        lane = lax.broadcasted_iota(jnp.int32, (quarter, LANES), 1)
        dead = (lane == 0) & (row >= length - j * quarter)
        bias = jnp.where(dead, NEG, 0.0).astype(BF)
        for p in range(HEADS // 2):
            k_s[j, :, 2 * p * LANES : (2 * p + 1) * LANES] = keys[:, p * LANES : (p + 1) * LANES]
            k_s[j, :, (2 * p + 1) * LANES : (2 * p + 2) * LANES] = bias
        v_s[j] = lax.dot_general(wv[...], normed, dims_nt, preferred_element_type=F32).astype(BF)


    def queries(slot):
        q_t = lax.dot_general(wq[...], normed_s[...], dims_nt, preferred_element_type=F32)
        q_t = (q_t * SCORE_SCALE).astype(BF)
        zero = jnp.zeros((head_dim, quarter), BF)
        one_row = lax.broadcasted_iota(jnp.int32, (LANES, quarter), 0) == 0
        one_row = jnp.where(one_row, 1.0, 0.0).astype(BF)
        for h in range(HEADS):
            mine = q_t[h * head_dim : (h + 1) * head_dim]
            pair = (mine, zero) if h % 2 == 0 else (zero, mine)
            qm[slot, h] = jnp.concatenate(pair + (one_row,), axis=0)
        m_s[slot] = jnp.full(m_s.shape[1:], NEG, F32)
        l_s[slot] = jnp.zeros(l_s.shape[1:], F32)
        acc[slot] = jnp.zeros(acc.shape[1:], F32)

    def step(t, carry):
        j = order(t)

        @pl.when(j <= hi)
        def _():
            arrive(j)
            project(j)

        def query_step(slot, carry):
            q = query_of(slot)
            @pl.when(j == q)
            def _():
                queries(slot)

            top_q = q == cols - 1
            late = is_inner & (q == cols // 2 - 1)
            ready = jnp.where(late, t == cols - 1, j == q)
            fresh = jnp.where(top_q, 1, q + 1)
            count = jnp.where(ready, fresh, jnp.where(top_q & (j < q), 1, 0))
            first = jnp.where(late, q, j)
            done = jnp.where(top_q, t == cols - 1, ready)

            def unit(i, carry):
                key = first - i

                @pl.when(key == q)
                def _():
                    attend(slot, key, True)

                @pl.when(key < q)
                def _():
                    attend(slot, key, False)

                return carry

            lax.fori_loop(0, count, unit, 0)

            @pl.when(done)
            def _():
                for p in range(2):
                    cut = slice(p * half, (p + 1) * half)
                    att_t = acc[slot, :, :, cut] / l_s[slot, :, :, cut]
                    attended = att_t.reshape(HEADS * head_dim, half).T.astype(BF)
                    rows_in = [ebuf[s, q, cut] for s in range(cols)]
                    hidden = jnp.concatenate(rows_in, axis=1).astype(F32) + jnp.dot(
                        attended, wo[...], preferred_element_type=F32
                    )
                    hidden = hidden.astype(BF)

                    @pl.when(q == me)
                    def _():
                        hbuf[hist, cut] = hidden

                    @pl.when(q != me)
                    def _():
                        hstage[slot, cut] = hidden
                        hidden_copy(slot, p).start()

            return carry

        @pl.when(j <= hi)
        def _():
            lax.fori_loop(0, 3, query_step, 0)

        return carry

    lax.fori_loop(0, cols, step, 0)

    def mlp(i, carry):
        first = jnp.where(falling | is_inner, hist, other)
        h = jnp.where(i < 2, first, batch - 1 - first)
        p = lax.rem(i, 2)
        part = pl.ds(pl.multiple_of(p * half, half), half)

        local = (query_of(0) == me) | (query_of(1) == me) | (query_of(2) == me)

        @pl.when((h != hist) | ~local)
        def _():
            hidden_arrival(h, p).wait_recv()

        hidden = hbuf[h, part, :].astype(F32)
        normed_two = rms_norm(hidden, gain2[...]).astype(BF)
        ff = wd.shape[0]
        tile = 1024
        total = hidden
        for f in range(0, ff, tile):
            gate = jnp.dot(normed_two, wi[:, f : f + tile], preferred_element_type=F32)
            up = jnp.dot(normed_two, wi[:, ff + f : ff + f + tile], preferred_element_type=F32)
            act = (gate / (1.0 + jnp.exp(-gate)) * up).astype(BF)
            total = total + jnp.dot(act, wd[f : f + tile, :], preferred_element_type=F32)
        out_v[i] = total.astype(BF)
        out_copy(i).start()
        return carry

    def out_copy(i):
        first = jnp.where(falling | is_inner, hist, other)
        h = jnp.where(i < 2, first, batch - 1 - first)
        part = pl.ds(pl.multiple_of(lax.rem(i, 2) * half, half), half)
        return pltpu.make_async_copy(out_v.at[i], out_ref.at[h, part], out_sem.at[i])

    lax.fori_loop(0, 2 * batch, mlp, 0)
    for i in range(2 * batch):
        out_copy(i).wait()
    for j in range(cols):
        far_copy(j).wait_send()

        @pl.when(j <= mate_hi)
        def _():
            mate_copy(j).wait_send()

        for s in range(cols):

            @pl.when(is_inner & (s // group == other) & (j == 0))
            def _():
                pass_copy(s, j).wait_send()

    for slot in range(3):

        @pl.when((query_of(slot) != me) & (query_of(slot) >= 0))
        def _():
            for p in range(2):
                hidden_copy(slot, p).wait_send()

    for off in range(1, cols):
        ids_copy(lax.rem(me + off, cols)).wait_send()
    over_rows(lambda r: req_copy(r).wait_send())
    for p in range(2):
        over_rows(lambda r: row_copy(r, p).wait_send())


def whole_call(rows, cols, cap, token_ids, lengths, table, gain1, gain2, w_qkv, w_out, w_in, w_down):
    batch, quarter = token_ids.shape
    tokens = batch * quarter * cols
    lines = tokens // LANES
    block_rows, width = table.shape
    d = width * cols
    head_dim = d // HEADS
    assert batch == 2 and cols == 2 * batch and rows % 2 == 0
    assert block_rows & (block_rows - 1) == 0 and rows * cap <= block_rows
    groups = -(-cap // (8 * LANES)) * 8
    any_spec = pl.BlockSpec(memory_space=pl.ANY)
    vmem = pl.BlockSpec(memory_space=pltpu.VMEM)
    smem = pl.BlockSpec(memory_space=pltpu.SMEM)
    dma = pltpu.SemaphoreType.DMA
    i32 = jnp.int32
    return pl.pallas_call(
        functools.partial(whole_kernel, rows, cols, cap),
        out_shape=jax.ShapeDtypeStruct((batch, quarter, d), BF),
        in_specs=[vmem, smem, any_spec, vmem, vmem] + [any_spec] * 4,
        out_specs=any_spec,
        scratch_shapes=[
            pltpu.VMEM((cols, batch, quarter), i32),
            pltpu.VMEM((lines, LANES), i32),
            pltpu.VMEM((lines, LANES), i32),
            pltpu.SMEM((lines, LANES), i32),
            pltpu.VMEM((rows * groups, tokens), BF),
            pltpu.VMEM((2 * LANES, tokens), BF),
            pltpu.VMEM((rows, groups, LANES), i32),
            pltpu.VMEM((rows, groups, LANES), i32),
            pltpu.SMEM((rows, groups, LANES), i32),
            pltpu.VMEM((block_rows, width), BF),
            pltpu.VMEM((block_rows, width), F32),
            pltpu.VMEM((rows, cap, width), BF),
            pltpu.VMEM((rows, cap, width), BF),
            pltpu.VMEM((LANES, width), F32),
            pltpu.VMEM((cols, quarter, width), BF),
            pltpu.VMEM((cols, cols, quarter, width), BF),
            pltpu.VMEM((batch, quarter, d), BF),
            pltpu.VMEM((3, quarter, d), BF),
            pltpu.VMEM(w_qkv.shape, BF),
            pltpu.VMEM(w_out.shape, BF),
            pltpu.VMEM(w_in.shape, BF),
            pltpu.VMEM(w_down.shape, BF),
            pltpu.VMEM((d, d), BF),
            pltpu.VMEM((d, d), BF),
            pltpu.VMEM((3, HEADS, 4 * head_dim, quarter), BF),
            pltpu.VMEM((cols, quarter, 2 * d), BF),
            pltpu.VMEM((cols, d, quarter), BF),
            pltpu.VMEM((3, HEADS, 1, quarter), F32),
            pltpu.VMEM((3, HEADS, 1, quarter), F32),
            pltpu.VMEM((3, HEADS, head_dim, quarter), F32),
            pltpu.VMEM((2, quarter, quarter), F32),
            pltpu.VMEM((2 * batch, quarter // 2, d), BF),
            pltpu.VMEM((quarter, d), BF),
            dma((cols,)),
            dma((cols,)),
            dma((rows,)),
            dma((rows,)),
            dma((rows, 2)),
            dma((rows, 2)),
            dma((4,)),
            dma((2,)),
            dma((2, cols)),
            dma((cols, cols)),
            dma((cols, cols)),
            dma((3, 2)),
            dma((batch, 2)),
            dma((4,)),
            dma((2 * batch,)),
        ],
        compiler_params=pltpu.CompilerParams(
            collective_id=0, has_side_effects=True, vmem_limit_bytes=63 * 1024 * 1024
        ),
    )(token_ids, lengths, table, gain1.reshape(1, d), gain2.reshape(1, d), w_qkv, w_out, w_in, w_down)


def local(token_ids, lengths, table, attn_gain, w_qkv, w_out, mlp_gain, w_in, w_down):
    batch_dev, quarter = token_ids.shape
    col_count = lax.axis_size("cols")
    row_count = lax.axis_size("rows")
    token_count = batch_dev * quarter * col_count
    capacity = -(-(8 * token_count // (3 * row_count)) // 32) * 32
    return whole_call(
        row_count, col_count, capacity, token_ids, lengths, table,
        attn_gain, mlp_gain, w_qkv, w_out, w_in, w_down,
    )


def solution(mesh):
    in_specs = (P("rows", "cols"), P("rows"), P("rows", "cols"), P(), P(), P(), P(), P(), P())
    out_specs = P("rows", "cols", None)
    return jax.shard_map(local, mesh=mesh, in_specs=in_specs, out_specs=out_specs, check_vma=False)
```
